32 devices in a mesh: lat: 4 (over x, core), lon: 8 (over z, y).
Axes of the slice: x: 2, y: 2, z: 4, core: 2. Of those that a mesh axis runs over, the one named last changes fastest.
Arguments:
- zonal_wind: float32 [16, 32, 2048], P(None, 'lat', 'lon'), may hold values from -0.45 to 0.45
- merid_wind: float32 [16, 32, 2048], P(None, 'lat', 'lon'), may hold values from -0.45 to 0.45
- operator_rows: float32 [8, 64], replicated, may hold values from -1.5 to 1.5
- innovation: float32 [131072], P(('lat', 'lon')), may hold values from -6 to 6
- error_weight: float32 [131072], P(('lat', 'lon')), may hold values from 0.25 to 4
- interp_weight: float32 [4, 131072], P(None, ('lat', 'lon')), may hold values from 0.05 to 1
- obs_slot: int32 [4, 131072], P(None, ('lat', 'lon')), may hold values from 0 to 2047
- block_count: int32 [1024], P(('lat', 'lon')), may hold values from 1 to 128
- block_type: int32 [1024], P(('lat', 'lon')), may hold values from 0 to 7
- block_window: int32 [1024], P(('lat', 'lon')), may hold values from 0 to 2
- send_cols: int32 [32, 2048], P(('lat', 'lon')), may hold values from 0 to 2047
Outputs:
- increment: float32 [4, 16, 32, 2048], P(None, None, 'lat', 'lon')
- residual: float32 [4, 16, 32, 2048], P(None, None, 'lat', 'lon')
The draws below stay inside these ranges and needn't reach their ends.
Inputs may be any that keep to these rules, and one draw needn't show every extreme that they name: `obs_slot`: an index into the 2048 slots that the observation's own device receives: slot s * 64 + q comes from device s. `send_cols`: entry r * 64 + q of device s's row is a local cell of device s, row-major over 8 x 256, sent to slot q of device r. `block_count`: rows of a block at or past its count are padding and observe nothing.
All inputs are finite; a program needn't handle non-finite values.
Results may differ from the reference program's by a relative error of at most 0.00025.
Values sent between devices are 32-bit elements; how exact they have to be, the bound alone decides.
No kernel may reach another device: no remote copies, remote signals or barrier semaphores. Data moves between devices by JAX's collectives and lax.ppermute only.
A program may use at most 128 MiB of HBM per device.

```python
import math
import jax
import jax.numpy as jnp
from jax import lax

VARS = 4
LEV = 16
TYPES = 8
KPTS = 4
WIN = 3
STEP_WIN = 2
ITERS = 2
BLOCK_ROWS = 128
CLAT = 8
CLON = 256
RECV = 2048
CHANNELS = 64
NLAT = 32
NLON = 2048
SLOTS = 64
NOBS_DEV = 4096
NOBS = 131072
NBLK = 1024
N_LAT = 4
N_LON = 8


def place_ends(result, own_key, smallest, largest):
    longest = result.shape.index(max(result.shape))
    spots = []
    for shift in (0, 1):
        where = [jax.random.randint(jax.random.fold_in(own_key, axis), (), 0, length) for axis, length in enumerate(result.shape)]
        where[longest] = (where[longest] + shift) % result.shape[longest]
        spots.append(tuple(where))
    return result.at[spots[0]].set(smallest).at[spots[1]].set(largest)


def level_of(own_key, extent, pieces, smallest, top_value):
    def one(dim, parts):
        steps = jax.random.uniform(jax.random.fold_in(jax.random.fold_in(own_key, 6), dim), (parts,), jnp.float32, smallest / len(pieces), top_value / len(pieces))
        return jnp.repeat(jnp.exp(steps), extent[dim] // parts).reshape((-1,) + (1,) * (len(extent) - dim - 1))

    loudness = one(*pieces[0])
    for cut in pieces[1:]:
        loudness = loudness * one(*cut)
    return loudness


def normal_values(stream_key, shape, spread, most, split=(), held_as=jnp.bfloat16):
    entries = jax.random.normal(stream_key, shape, jnp.float32) * spread
    if len(split) > 0:
        entries = level_of(stream_key, shape, split, -0.22, 0.18) * entries
    return jnp.clip(entries, min=-most, max=most).astype(held_as)


def setup_inputs(seed: int = 0) -> dict:
    seeds = jax.random.split(jax.random.key(seed), 12)
    zonal_wind = jnp.clip(jax.random.uniform(seeds[0], (LEV, NLAT, NLON), jnp.float32, -0.45, 0.45) * level_of(seeds[0], (LEV, NLAT, NLON), ((1, 4), (2, 8)), -0.4, 0.0), -0.45, 0.45)
    merid_wind = jnp.clip(jax.random.uniform(seeds[1], (LEV, NLAT, NLON), jnp.float32, -0.45, 0.45) * level_of(seeds[1], (LEV, NLAT, NLON), ((1, 4), (2, 8)), -0.4, 0.0), -0.45, 0.45)
    operator_rows = normal_values(seeds[2], (TYPES, CHANNELS), (CHANNELS // 4) ** -0.5, 1.5, (), jnp.float32)
    innovation = normal_values(seeds[3], (NOBS,), 1.0, 6.0, ((0, 32),), jnp.float32)
    error_weight = jnp.clip(jnp.exp(math.log(4.0) - 2.7725887 * jax.random.uniform(seeds[4], (NOBS,), jnp.float32) ** level_of(seeds[4], (NOBS,), ((0, 32),), -0.2, 0.2)), 0.25, 4.0)
    interp_weight = jnp.clip(0.05 + 0.95 * jax.random.uniform(seeds[5], (KPTS, NOBS), jnp.float32) ** level_of(seeds[5], (KPTS, NOBS), ((1, 32),), -0.2, 0.2), 0.05, 1.0)
    obs_slot = place_ends(jax.random.randint(seeds[6], (KPTS, NOBS), 0, RECV), jax.random.fold_in(seeds[6], 1), 0, RECV - 1).astype(jnp.int32)
    block_count = place_ends(jax.random.randint(seeds[7], (NBLK,), 1, BLOCK_ROWS + 1), jax.random.fold_in(seeds[7], 1), 1, BLOCK_ROWS).astype(jnp.int32)
    block_type = place_ends(jax.random.randint(seeds[8], (NBLK,), 0, TYPES), jax.random.fold_in(seeds[8], 1), 0, TYPES - 1).astype(jnp.int32)
    block_window = place_ends(jax.random.randint(seeds[9], (NBLK,), 0, WIN), jax.random.fold_in(seeds[9], 1), 0, WIN - 1).astype(jnp.int32)
    send_cols = place_ends(jax.random.randint(seeds[10], (N_LAT * N_LON, RECV), 0, CLAT * CLON), jax.random.fold_in(seeds[10], 1), 0, (CLAT * CLON) - 1).astype(jnp.int32)
    return dict(zonal_wind=zonal_wind, merid_wind=merid_wind, operator_rows=operator_rows, innovation=innovation, error_weight=error_weight, interp_weight=interp_weight, obs_slot=obs_slot, block_count=block_count, block_type=block_type, block_window=block_window, send_cols=send_cols)


HIGH = lax.Precision.HIGHEST


def from_below(field):
    padded = jnp.pad(field, ((0, 0), (0, 0), (1, 0), (0, 0)))
    return padded[:, :, :-1]


def from_above(field):
    padded = jnp.pad(field, ((0, 0), (0, 0), (0, 1), (0, 0)))
    return padded[:, :, 1:]


def reference(zonal_wind, merid_wind, operator_rows, innovation, error_weight, interp_weight, obs_slot, block_count, block_type, block_window, send_cols):
    keep_rate = 1.0 - jnp.abs(zonal_wind) - jnp.abs(merid_wind)
    from_west = jnp.maximum(zonal_wind, 0.0)
    from_east = jnp.minimum(zonal_wind, 0.0)
    from_south = jnp.maximum(merid_wind, 0.0)
    from_north = jnp.minimum(merid_wind, 0.0)
    devices = N_LAT * N_LON
    ncell = NLAT * NLON
    channels = VARS * LEV
    source = jnp.arange(devices, dtype=jnp.int32)[:, None]
    row_global = (source // N_LON) * CLAT + send_cols // CLON
    col_global = (source % N_LON) * CLON + send_cols % CLON
    global_cell = (row_global * NLON + col_global).reshape(devices, devices, SLOTS)
    global_cell = jnp.transpose(global_cell, (1, 0, 2)).reshape(devices * RECV)
    owner = (jnp.arange(NOBS, dtype=jnp.int32) // NOBS_DEV)[None, :]
    cell = global_cell[owner * RECV + obs_slot]
    live = (jnp.arange(BLOCK_ROWS, dtype=jnp.int32)[None, :] < block_count[:, None]).reshape(NOBS)
    weight_live = error_weight * live.astype(jnp.float32)
    row_type = jnp.broadcast_to(block_type[:, None], (NBLK, BLOCK_ROWS)).reshape(NOBS)
    row_window = jnp.broadcast_to(block_window[:, None], (NBLK, BLOCK_ROWS)).reshape(NOBS)
    flat_index = ((row_window * TYPES + row_type)[None, :] * ncell + cell).astype(jnp.int32)

    def tangent_step(field):
        west = jnp.roll(field, 1, axis=3)
        east = jnp.roll(field, -1, axis=3)
        return keep_rate * field + from_west * west - from_east * east + from_south * from_below(field) - from_north * from_above(field)

    def adjoint_step(field):
        return keep_rate * field + jnp.roll(from_west * field, -1, axis=3) - jnp.roll(from_east * field, 1, axis=3) + from_above(from_south * field) - from_below(from_north * field)

    def forward_model(field):
        states = [field]
        for _ in range(WIN - 1):
            for _ in range(STEP_WIN):
                field = tangent_step(field)
            states.append(field)
        return states

    def observe(states):
        projected = jnp.stack([jnp.dot(operator_rows, state.reshape(channels, ncell), precision=HIGH) for state in states])
        picked = projected.reshape(-1)[flat_index]
        return jnp.sum(interp_weight * picked, axis=0)

    def adjoint_model(weighted):
        terms = (interp_weight * weighted[None, :]).reshape(-1)
        summed = jax.ops.segment_sum(terms, flat_index.reshape(-1), num_segments=WIN * TYPES * ncell).reshape(WIN, TYPES, ncell)
        forcing = [jnp.dot(operator_rows.T, summed[window], precision=HIGH).reshape(VARS, LEV, NLAT, NLON) for window in range(WIN)]
        field = forcing[WIN - 1]
        for window in range(WIN - 2, -1, -1):
            for _ in range(STEP_WIN):
                field = adjoint_step(field)
            field = field + forcing[window]
        return field

    def hessian(direction):
        return direction + adjoint_model(weight_live * observe(forward_model(direction)))

    right = adjoint_model(weight_live * innovation)
    increment = jnp.zeros_like(right)
    residual = right
    direction = right
    norm_now = jnp.sum(residual * residual)
    for _ in range(ITERS):
        image = hessian(direction)
        alpha = norm_now / jnp.sum(direction * image)
        increment = increment + alpha * direction
        residual = residual - alpha * image
        norm_next = jnp.sum(residual * residual)
        direction = residual + (norm_next / norm_now) * direction
        norm_now = norm_next
    return increment, residual
```

```python
import functools

import jax
import jax.numpy as jnp
from jax import lax
from jax.experimental import pallas as pl
from jax.experimental.pallas import tpu as pltpu
from jax.sharding import PartitionSpec as P

WIN = 3
STEP_WIN = 2
ITERS = 2
BLOCK_ROWS = 128
LANES = 128
SUB = 8
REACH = STEP_WIN * (WIN - 1)
HALO = 2 * REACH
AXES = ("lat", "lon")
F32 = jnp.float32
BF16 = jnp.bfloat16
NT = (((1,), (1,)), ((), ()))


def log2(n):
    assert n & (n - 1) == 0
    return n.bit_length() - 1


def iota(shape, dim):
    return lax.broadcasted_iota(jnp.int32, shape, dim)


def halves(x):
    top = x.astype(BF16).astype(F32)
    return top, x - top


def dot(a, b):
    return jnp.dot(a, b, preferred_element_type=F32)


class Packing:
    def __init__(self, devices, recv):
        self.devices = devices
        self.recv = recv
        self.slots = recv // devices
        assert self.slots <= LANES and recv % LANES == 0
        self.per = LANES // self.slots
        self.tiles = WIN // self.per + 1
        self.rows = self.tiles * SUB
        self.spare_tile, self.spare_group = WIN // self.per, WIN % self.per
        self.group_bits = log2(self.slots)

    def group(self, shape):
        return iota(shape, len(shape) - 1) >> self.group_bits

    def spare(self, row):
        lane = iota(row.shape, 1)
        first = lane == self.spare_group * self.slots
        return jnp.sum(jnp.where(first, row, 0.0), axis=1, keepdims=True)

    def write(self, out_ref, typed, spare, tile):
        group = self.group((SUB, LANES))
        for d in range(self.per):
            device = tile * self.per + d
            for part in range(self.tiles):
                chunk = jnp.zeros((SUB, LANES), F32)
                for g in range(self.per):
                    w = part * self.per + g
                    if w < WIN:
                        piece = turn(typed[w], (g - d) * self.slots)
                    elif w == WIN:
                        piece = spare
                    else:
                        continue
                    chunk = jnp.where(group == g, piece, chunk)
                at = (device * self.tiles + part) * SUB
                out_ref[at : at + SUB, :] = chunk

    def read(self, ref, w, tile):
        group = self.group((SUB, LANES))
        part, g = w // self.per, w % self.per
        found = jnp.zeros((SUB, LANES), F32)
        for d in range(self.per):
            at = ((tile * self.per + d) * self.tiles + part) * SUB
            piece = turn(ref[at : at + SUB, :], (d - g) * self.slots)
            found = jnp.where(group == d, piece, found)
        return found


def turn(x, shift):
    shift %= x.shape[-1]
    return pltpu.roll(x, shift, len(x.shape) - 1) if shift else x


def observe_kernel(pack, mode, count_ref, type_ref, window_ref, *refs):
    if mode == "right":
        slot_ref, weight_ref, error_ref, value_ref, out_ref, total = refs
    else:
        if mode == "start":
            recv_ref, slot_ref, weight_ref, error_ref = refs[:4]
            refs = refs[4:]
        else:
            recv_ref, slot_ref, weight_ref, error_ref, value_ref, before_ref = refs[:6]
            refs = refs[6:]
        out_ref, observed_ref, scalar_ref, total, table = refs
    points = slot_ref.shape[0]
    blocks = error_ref.shape[0]
    devices = pack.devices
    wide = points * BLOCK_ROWS
    spare = pack.spare_tile * SUB
    total[...] = jnp.zeros_like(total)
    if mode != "right":
        for j in range(pack.rows):
            table[j] = recv_ref[pl.ds(j, devices, stride=pack.rows), :]
        norm = pack.spare(jnp.sum(table[spare], axis=0, keepdims=True))
        if mode == "start":
            ratio, square = jnp.zeros_like(norm), norm
        else:
            cross = pack.spare(jnp.sum(table[spare + 1], axis=0, keepdims=True))
            ratio = norm / before_ref[0:1, 0:1]
            square = norm + 2.0 * ratio * cross + ratio * ratio * before_ref[2:3, 0:1]
        row = iota((SUB, LANES), 0)
        scalar_ref[...] = jnp.where(row == 0, norm, jnp.where(row == 1, ratio, square))

    def one(b, energy):
        window = window_ref[b]
        j = (window >> log2(pack.per)) * SUB + type_ref[b]
        shift = (window & (pack.per - 1)) * pack.slots
        lanes = pl.ds(pl.multiple_of(b * BLOCK_ROWS, BLOCK_ROWS), BLOCK_ROWS)
        slot = slot_ref[:, lanes]
        weight = weight_ref[:, lanes]
        device = slot >> pack.group_bits
        lane = (slot & (pack.slots - 1)) + shift
        ids = iota((LANES, BLOCK_ROWS), 0)
        pick = jnp.concatenate(
            [jnp.where(ids == lane[k : k + 1, :], 1.0, 0.0) for k in range(points)], axis=1
        ).astype(BF16)
        device = jnp.concatenate([device[k : k + 1, :] for k in range(points)], axis=1)
        weight = jnp.concatenate([weight[k : k + 1, :] for k in range(points)], axis=1)
        owner = iota((devices, wide), 0) == device
        if mode == "right":
            value = value_ref[pl.ds(b, 1), :]
        else:
            top, rest = halves(table[j])
            both = dot(jnp.concatenate([top, rest], axis=0).astype(BF16), pick)
            both = both[:devices] + both[devices:]
            found = jnp.sum(jnp.where(owner, both, 0.0), axis=0, keepdims=True) * weight
            value = found[:, :BLOCK_ROWS]
            for k in range(1, points):
                value = value + found[:, k * BLOCK_ROWS : (k + 1) * BLOCK_ROWS]
            if mode == "next":
                value = value + ratio * value_ref[pl.ds(b, 1), :]
            observed_ref[pl.ds(b, 1), :] = value
        live = iota((1, BLOCK_ROWS), 1) < count_ref[b]
        weighted = jnp.where(live, error_ref[pl.ds(b, 1), :], 0.0) * value
        spread = jnp.concatenate([weighted] * points, axis=1) * weight
        top, rest = halves(jnp.where(owner, spread, 0.0))
        both = lax.dot_general(
            jnp.concatenate([top, rest], axis=0).astype(BF16),
            pick,
            NT,
            preferred_element_type=F32,
        )
        total[j] += both[:devices] + both[devices:]
        return energy + weighted * value

    energy = lax.fori_loop(0, blocks, one, jnp.zeros((1, BLOCK_ROWS), F32), unroll=4)
    energy = jnp.sum(energy, axis=1, keepdims=True)
    for j in range(pack.rows):
        chunk = total[j]
        if j == spare:
            chunk = jnp.where(pack.group((devices, LANES)) == pack.spare_group, energy, chunk)
        out_ref[pl.ds(j, devices, stride=pack.rows), :] = chunk


def collect_kernel(pack, lat_cells, with_winds, *refs):
    if with_winds:
        recv_ref, send_ref, zonal_ref, merid_ref = refs[:4]
        refs = refs[4:]
    else:
        recv_ref, send_ref = refs[:2]
        refs = refs[2:]
    main_ref, west_ref, east_ref, scalar_ref = refs[:4]
    lon_cells = main_ref.shape[2]
    cols = lon_cells // LANES
    tiles = pack.recv // LANES
    send = send_ref[...]
    pick = jnp.where(iota((LANES, pack.recv), 0) == (send & (LANES - 1)), 1.0, 0.0).astype(BF16)
    high = send >> log2(LANES)
    strips = {}

    def note(slab, left, right):
        at = slab * HALO
        q, s = at // LANES, at % LANES
        lane = iota((SUB, LANES), 1)
        inside = (lane >= s) & (lane < s + HALO)
        west, east = strips.get(q, (jnp.zeros((SUB, LANES), F32),) * 2)
        west = jnp.where(inside, turn(left, s), west)
        east = jnp.where(inside, turn(right, s - (LANES - HALO)), east)
        strips[q] = (west, east)

    for w in range(WIN):
        typed = jnp.concatenate([pack.read(recv_ref, w, t) for t in range(tiles)], axis=1)
        masked = []
        for part in halves(typed):
            masked += [
                jnp.where(high == h, part, 0.0) for h in range(lat_cells * cols)
            ]
        both = lax.dot_general(
            jnp.concatenate(masked, axis=0).astype(BF16), pick, NT, preferred_element_type=F32
        )
        count = lat_cells * cols * SUB
        forcing = both[:count] + both[count:]
        for row in range(lat_cells):
            slab = w * lat_cells + row
            pieces = [
                forcing[(row * cols + c) * SUB : (row * cols + c + 1) * SUB] for c in range(cols)
            ]
            for c in range(cols):
                main_ref[slab, :, c * LANES : (c + 1) * LANES] = pieces[c]
            note(slab, pieces[0], pieces[-1])
    if with_winds:
        slab = WIN * lat_cells
        levels = zonal_ref.shape[0] // lat_cells
        held = refs[4:]
        for ref in (zonal_ref, merid_ref):
            for c in range(cols):
                held[c][...] = ref[:, c * LANES : (c + 1) * LANES]
            for row in range(lat_cells):
                for part in range(levels // SUB):
                    at = pl.ds(part * SUB * lat_cells + row, SUB, stride=lat_cells)
                    pieces = [held[c][at, :] for c in range(cols)]
                    for c in range(cols):
                        main_ref[slab, :, c * LANES : (c + 1) * LANES] = pieces[c]
                    note(slab, pieces[0], pieces[-1])
                    slab += 1
    for q in range(west_ref.shape[1] // LANES):
        west, east = strips[q]
        west_ref[:, q * LANES : (q + 1) * LANES] = west
        east_ref[:, q * LANES : (q + 1) * LANES] = east
    row = recv_ref[pl.ds(pack.spare_tile * SUB, pack.devices, stride=pack.rows), :]
    energy = pack.spare(jnp.sum(row, axis=0, keepdims=True))
    scalar_ref[...] = jnp.broadcast_to(energy, scalar_ref.shape)


def model_kernel(pack, mode, dims, edge_ref, *refs):
    layers, levels, lat_cells, lon_cells = dims
    channels = layers * levels
    rows = lat_cells + 2 * HALO
    cols = lon_cells // LANES
    width = lon_cells + LANES
    refs = list(refs)

    def take(count):
        got = refs[:count]
        del refs[:count]
        return got

    mains = take(3)
    strips = [take(2), take(2), take(2)]
    into_ref, back_ref = take(2)
    if mode != "right":
        (winds,) = take(1)
        energy_ref, scalar_ref, residual_ref = take(3)
    if mode == "last":
        (energy0_ref, scalar0_ref, first_ref) = take(3)
        increment_out, residual_out = take(2)
    else:
        (send_ref,) = take(1)
        out_ref, state_out = take(2)
        if mode == "right":
            (winds,) = take(1)
        (picked,) = take(1)
    fields = take(2)
    forced, coef = take(2)
    ends = refs

    lane = iota((SUB, LANES), 1)

    def assemble(slab, block):
        main = mains[block]
        east, west = strips[block]
        q, s = slab * HALO // LANES, slab * HALO % LANES
        right = turn(east[:, q * LANES : (q + 1) * LANES], -s)
        left = turn(west[:, q * LANES : (q + 1) * LANES], LANES - HALO - s)
        edge = jnp.where(lane < HALO, right, jnp.where(lane >= LANES - HALO, left, 0.0))
        return jnp.concatenate([main[slab], edge], axis=1)

    def source(e):
        at = e - HALO
        if at < 0:
            return 0, lat_cells + at
        if at < lat_cells:
            return 1, at
        return 2, at - lat_cells

    for w in range(WIN):
        trim = STEP_WIN * (WIN - 1 - w)
        for e in range(trim, rows - trim):
            block, row = source(e)
            forced[w, e] = assemble(w * lat_cells + row, block)
    if mode == "right":
        for which in range(2):
            for e in range(rows):
                block, row = source(e)
                for part in range(levels // SUB):
                    slab = WIN * lat_cells + (which * lat_cells + row) * (levels // SUB) + part
                    winds[which, e, part * SUB : (part + 1) * SUB, :] = assemble(slab, block)

    def prepare(e, carry):
        u, v = winds[0, e], winds[1, e]
        coef[0, e] = 1.0 - jnp.abs(u) - jnp.abs(v)
        coef[1, e] = jnp.maximum(u, 0.0)
        coef[2, e] = jnp.maximum(-u, 0.0)
        coef[3, e] = jnp.maximum(v, 0.0)
        coef[4, e] = jnp.maximum(-v, 0.0)
        return carry

    lax.fori_loop(0, rows, prepare, 0)

    into = into_ref[...]
    top, rest = halves(into)
    into = jnp.where(iota(into.shape, 1) < 2 * SUB, top, rest).astype(BF16)

    def force(w, e):
        top, rest = halves(forced[w, e])
        return dot(into, jnp.concatenate([top, rest, top, rest], axis=0).astype(BF16))

    def pieces(part):
        level = slice(part * SUB, (part + 1) * SUB)
        return level, [
            slice(v * levels + part * SUB, v * levels + (part + 1) * SUB) for v in range(layers)
        ]

    def adjoint(field, e, put, extra=None):
        for part in range(levels // SUB):
            level, chans = pieces(part)
            keep, west, east = coef[0, e, level], coef[1, e, level], coef[2, e, level]
            south, north = coef[3, e + 1, level], coef[4, e - 1, level]
            for chan in chans:
                here = field[e, chan]
                result = (
                    keep * here
                    + turn(west * here, -1)
                    + turn(east * here, 1)
                    + south * field[e + 1, chan]
                    + north * field[e - 1, chan]
                )
                if extra is not None:
                    result = result + extra[chan]
                put(chan, result)

    def tangent(field, e, put):
        for part in range(levels // SUB):
            level, chans = pieces(part)
            keep, west, east = coef[0, e, level], coef[1, e, level], coef[2, e, level]
            south, north = coef[3, e, level], coef[4, e, level]
            for chan in chans:
                here = field[e, chan]
                put(
                    chan,
                    keep * here
                    + west * turn(here, 1)
                    + east * turn(here, -1)
                    + south * field[e - 1, chan]
                    + north * field[e + 1, chan],
                )

    def put_in(field, e):
        def put(chan, value):
            field[e, chan] = value

        return put

    def begin(e, carry):
        fields[0][e] = force(WIN - 1, e)
        return carry

    lax.fori_loop(0, rows, begin, 0)
    now = 0
    for step in range(1, REACH):
        old, new = fields[now], fields[1 - now]
        w = WIN - 1 - step // STEP_WIN if step % STEP_WIN == 0 else None

        def body(e, carry, old=old, new=new, w=w):
            extra = None if w is None else force(w, e)
            adjoint(old, e, put_in(new, e), extra)
            return carry

        lax.fori_loop(step, rows - step, body, 0)
        now = 1 - now
    old, new = fields[now], fields[1 - now]

    if mode != "right":
        alpha = scalar_ref[0:1, 0:1] / (scalar_ref[2:3, 0:1] + energy_ref[0:1, 0:1])
        ratio = scalar_ref[1:2, 0:1]
    if mode == "last":
        alpha0 = scalar0_ref[0:1, 0:1] / (scalar0_ref[2:3, 0:1] + energy0_ref[0:1, 0:1])

        def finish(row, carry):
            e = row + HALO

            def put(chan, value):
                at = pl.ds(chan.start * lat_cells + row, SUB, stride=lat_cells)
                for c in range(cols):
                    part = slice(c * LANES, (c + 1) * LANES)
                    residual = residual_ref[row + REACH, chan, part]
                    first = first_ref[row + REACH, chan, part]
                    direction = residual + ratio * first
                    image = direction + value[:, part]
                    ends[c][at, :] = alpha0 * first + alpha * direction
                    ends[cols + c][at, :] = residual - alpha * image

            adjoint(old, e, put, force(0, e))
            return carry

        lax.fori_loop(0, lat_cells, finish, 0)
        for c in range(cols):
            part = slice(c * LANES, (c + 1) * LANES)
            increment_out[:, part] = ends[c][...]
            residual_out[:, part] = ends[cols + c][...]
        return

    def update(e, sums):
        valid = jnp.where(e < HALO, edge_ref[0], jnp.where(e >= HALO + lat_cells, edge_ref[1], 1))
        scale = valid.astype(F32)
        inside = jnp.where((e >= HALO) & (e < HALO + lat_cells), 1, 0).astype(F32)
        at = e - REACH
        sums = list(sums)

        def put(chan, value):
            value = value * scale
            if mode != "right":
                before = residual_ref[at, chan]
                value = before - alpha * (before + value)
            state_out[at, chan] = value
            new[e, chan] = value
            kept = value[:, :lon_cells] * inside
            sums[0] = sums[0] + kept * value[:, :lon_cells]
            if mode != "right":
                sums[1] = sums[1] + kept * before[:, :lon_cells]

        adjoint(old, e, put, force(0, e))
        return tuple(sums)

    zero = jnp.zeros((SUB, lon_cells), F32)
    sums = (zero,) if mode == "right" else (zero, zero)
    sums = lax.fori_loop(REACH, rows - REACH, update, sums)
    sums = [jnp.sum(jnp.sum(s, axis=1, keepdims=True), axis=0, keepdims=True) for s in sums]
    now = 1 - now

    back = back_ref[...]
    top, rest = halves(back)
    back = jnp.where(iota(back.shape, 0) < SUB, top, rest).astype(BF16)

    def look(field, w):
        def body(row, carry):
            top, rest = halves(field[row + HALO, :, :lon_cells])
            both = dot(back, jnp.concatenate([top, rest], axis=0).astype(BF16))
            typed = both[:SUB] + both[SUB:]
            for c in range(cols):
                at = pl.multiple_of(((w * lat_cells + row) * cols + c) * SUB, SUB)
                picked[pl.ds(at, SUB), :] = typed[:, c * LANES : (c + 1) * LANES]
            return carry

        lax.fori_loop(0, lat_cells, body, 0)

    look(fields[now], 0)
    for step in range(1, REACH + 1):
        old, new = fields[now], fields[1 - now]

        def body(e, carry, old=old, new=new):
            tangent(old, e, put_in(new, e))
            return carry

        lax.fori_loop(REACH + step, rows - REACH - step, body, 0)
        now = 1 - now
        if step % STEP_WIN == 0:
            look(fields[now], step // STEP_WIN)

    row = iota((SUB, LANES), 0)
    spare = jnp.where(row == 0, sums[0], 0.0)
    if mode != "right":
        spare = jnp.where(row == 1, sums[1], spare)
    top, rest = halves(picked[...])
    values = jnp.concatenate([top, rest], axis=1).astype(BF16)
    chunk = 2 * LANES
    parts = lat_cells * cols
    for c in range(pack.recv // chunk):
        send = send_ref[:, c * chunk : (c + 1) * chunk]
        pick = jnp.where(iota((LANES, chunk), 0) == (send & (LANES - 1)), 1.0, 0.0)
        pick = jnp.concatenate([pick, pick], axis=0).astype(BF16)
        high = send >> log2(LANES)
        every = dot(values, pick)
        typed = []
        for w in range(WIN):
            found = jnp.zeros((SUB, chunk), F32)
            for h in range(parts):
                at = (w * parts + h) * SUB
                found = jnp.where(high == h, every[at : at + SUB], found)
            typed.append(found)
        for t in range(chunk // LANES):
            lanes = slice(t * LANES, (t + 1) * LANES)
            pack.write(out_ref, [x[:, lanes] for x in typed], spare, c * (chunk // LANES) + t)


def call(kernel, out_shapes, args, scalars, scratch, limit=40):
    specs = [pl.BlockSpec(memory_space=pltpu.SMEM)] * scalars
    specs += [pl.BlockSpec(memory_space=pltpu.VMEM)] * (len(args) - scalars)
    return pl.pallas_call(
        kernel,
        out_shape=[jax.ShapeDtypeStruct(s, F32) for s in out_shapes],
        in_specs=specs,
        out_specs=[pl.BlockSpec(memory_space=pltpu.VMEM)] * len(out_shapes),
        scratch_shapes=[pltpu.VMEM(s, F32) for s in scratch],
        compiler_params=pltpu.CompilerParams(vmem_limit_bytes=limit << 20),
    )(*args)


def shards(
    zonal_wind,
    merid_wind,
    operator_rows,
    innovation,
    error_weight,
    interp_weight,
    obs_slot,
    block_count,
    block_type,
    block_window,
    send_cols,
):
    levels, lat_cells, lon_cells = zonal_wind.shape
    types, channels = operator_rows.shape
    layers = channels // levels
    n_lat, n_lon = lax.axis_size("lat"), lax.axis_size("lon")
    recv = send_cols.shape[1]
    blocks = block_count.shape[0]
    pack = Packing(n_lat * n_lon, recv)
    assert types == SUB and lat_cells >= HALO and lon_cells % LANES == 0
    dims = (layers, levels, lat_cells, lon_cells)
    rows, width = lat_cells + 2 * HALO, lon_cells + LANES
    chunks = (pack.devices * pack.rows, LANES)
    block_args = [block_count, block_type, block_window]
    rows_of = lambda x: x.reshape(blocks, BLOCK_ROWS)
    error = rows_of(error_weight)
    total = (pack.rows, pack.devices, LANES)
    band = lax.axis_index("lat")
    edges = jnp.stack([band > 0, band < n_lat - 1]).astype(jnp.int32)
    into = jnp.tile(operator_rows.T, (1, 4))
    back = jnp.tile(operator_rows, (2, 2))

    def exchange(x):
        x = x.reshape(pack.devices, pack.rows, LANES)
        x = lax.all_to_all(x, AXES, split_axis=0, concat_axis=0, tiled=True)
        return x.reshape(chunks)

    def send(x, up, right):
        pairs = [
            (i * n_lon + j, (i + up) * n_lon + (j + right) % n_lon)
            for i in range(n_lat)
            for j in range(n_lon)
            if 0 <= i + up < n_lat
        ]
        return lax.ppermute(x, AXES, pairs)

    def collect(received, with_winds):
        slabs = WIN * lat_cells
        args = [received, send_cols]
        if with_winds:
            slabs += 2 * lat_cells * (levels // SUB)
            args += [x.reshape(levels * lat_cells, lon_cells) for x in (zonal_wind, merid_wind)]
        strip = (SUB, -(-slabs * HALO // LANES) * LANES)
        main, west, east, energy = call(
            functools.partial(collect_kernel, pack, lat_cells, with_winds),
            [(slabs, SUB, lon_cells), strip, strip, (SUB, LANES)],
            args,
            0,
            [(levels * lat_cells, LANES)] * (lon_cells // LANES) if with_winds else [],
        )
        mains = [send(main, 1, 0), main, send(main, -1, 0)]
        strips = []
        for up in (1, 0, -1):
            strips += [send(west, up, -1), send(east, up, 1)]
        return mains + strips, energy

    def model(mode, halos, extra):
        ends = (channels * lat_cells, lon_cells)
        state = (lat_cells + 2 * REACH, channels, width)
        outs = [ends, ends] if mode == "last" else [chunks, state]
        scratch = [(rows, channels, width)] * 2
        scratch += [(WIN, rows, SUB, width), (5, rows, levels, width)]
        if mode == "right":
            outs += [(2, rows, levels, width)]
        if mode == "last":
            scratch += [(ends[0], LANES)] * (2 * lon_cells // LANES)
        if mode != "last":
            scratch = [(WIN * lat_cells * lon_cells // LANES * SUB, LANES)] + scratch
        return call(
            functools.partial(model_kernel, pack, mode, dims),
            outs,
            [edges, *halos, into, back, *extra],
            1,
            scratch,
        )

    def observe(mode, received, extra):
        outs, scratch = [chunks], [total]
        if mode != "right":
            outs += [(blocks, BLOCK_ROWS), (SUB, LANES)]
            scratch += [total]
        return call(
            functools.partial(observe_kernel, pack, mode),
            outs,
            block_args + received + [obs_slot, interp_weight, error] + extra,
            3,
            scratch,
        )

    assert ITERS == 2
    (chunk,) = observe("right", [], [rows_of(innovation)])
    halos, _ = collect(exchange(chunk), True)
    chunk, right, winds = model("right", halos, [send_cols])
    chunk, seen, scalar0 = observe("start", [exchange(chunk)], [])
    halos, energy0 = collect(exchange(chunk), False)
    chunk, residual = model("next", halos, [winds, energy0, scalar0, right, send_cols])
    chunk, seen, scalar1 = observe("next", [exchange(chunk)], [seen, scalar0])
    halos, energy1 = collect(exchange(chunk), False)
    ends = model(
        "last", halos, [winds, energy1, scalar1, residual, energy0, scalar0, right]
    )
    return tuple(x.reshape(layers, levels, lat_cells, lon_cells) for x in ends)


def solution(mesh):
    return jax.shard_map(
        shards,
        mesh=mesh,
        in_specs=(
            P(None, "lat", "lon"),
            P(None, "lat", "lon"),
            P(),
            P(("lat", "lon")),
            P(("lat", "lon")),
            P(None, ("lat", "lon")),
            P(None, ("lat", "lon")),
            P(("lat", "lon")),
            P(("lat", "lon")),
            P(("lat", "lon")),
            P(("lat", "lon"), None),
        ),
        out_specs=(P(None, None, "lat", "lon"), P(None, None, "lat", "lon")),
        check_vma=False,
    )
```

```python
import functools

import jax
import jax.numpy as jnp
from jax import lax
from jax.experimental import pallas as pl
from jax.experimental.pallas import tpu as pltpu
from jax.sharding import PartitionSpec as P

WIN = 3
STEP_WIN = 2
ITERS = 2
BLOCK_ROWS = 128
LANES = 128
SUB = 8
REACH = STEP_WIN * (WIN - 1)
HALO = 2 * REACH
AXES = ("lat", "lon")
F32 = jnp.float32
BF16 = jnp.bfloat16
NT = (((1,), (1,)), ((), ()))


def log2(n):
    assert n & (n - 1) == 0
    return n.bit_length() - 1


def iota(shape, dim):
    return lax.broadcasted_iota(jnp.int32, shape, dim)


def halves(x):
    top = x.astype(BF16).astype(F32)
    return top, x - top


def dot(a, b):
    return jnp.dot(a, b, preferred_element_type=F32)


def loop(low, high, step, body, carry=0):
    count = high - low
    while count % step:
        step -= 1

    def some(i, carry):
        for k in range(step):
            carry = body(low + i * step + k, carry)
        return carry

    return lax.fori_loop(0, count // step, some, carry)


def trims(halo):
    return [max(halo - STEP_WIN * (WIN - 1 - w), 0) for w in range(WIN)]


class Packing:
    def __init__(self, devices, recv):
        self.devices = devices
        self.recv = recv
        self.slots = recv // devices
        assert self.slots <= LANES and recv % LANES == 0
        self.per = LANES // self.slots
        self.tiles = WIN // self.per + 1
        self.rows = self.tiles * SUB
        self.spare_tile, self.spare_group = WIN // self.per, WIN % self.per
        self.group_bits = log2(self.slots)

    def group(self, shape):
        return iota(shape, len(shape) - 1) >> self.group_bits

    def spare(self, row):
        lane = iota(row.shape, 1)
        first = lane == self.spare_group * self.slots
        return jnp.sum(jnp.where(first, row, 0.0), axis=1, keepdims=True)

    def write(self, out_ref, typed, spare, tile):
        group = self.group((SUB, LANES))
        for d in range(self.per):
            device = tile * self.per + d
            for part in range(self.tiles):
                chunk = jnp.zeros((SUB, LANES), F32)
                for g in range(self.per):
                    w = part * self.per + g
                    if w < WIN:
                        piece = turn(typed[w], (g - d) * self.slots)
                    elif w == WIN:
                        piece = spare
                    else:
                        continue
                    chunk = jnp.where(group == g, piece, chunk)
                at = (device * self.tiles + part) * SUB
                out_ref[at : at + SUB, :] = chunk

    def read(self, ref, w, tile):
        group = self.group((SUB, LANES))
        part, g = w // self.per, w % self.per
        found = jnp.zeros((SUB, LANES), F32)
        for d in range(self.per):
            at = ((tile * self.per + d) * self.tiles + part) * SUB
            piece = turn(ref[at : at + SUB, :], (d - g) * self.slots)
            found = jnp.where(group == d, piece, found)
        return found


def turn(x, shift):
    shift %= x.shape[-1]
    return pltpu.roll(x, shift, len(x.shape) - 1) if shift else x


def observe_kernel(pack, mode, count_ref, type_ref, window_ref, *refs):
    if mode == "right":
        far = (count_ref, type_ref, window_ref) + refs[:4]
        out_ref, total = refs[4:6]
        near, done = refs[6:-1], refs[-1]
        copies = [
            pltpu.make_async_copy(src, dst, done.at[i])
            for i, (src, dst) in enumerate(zip(far, near))
        ]
        for copy in copies:
            copy.start()
        total[...] = jnp.zeros_like(total)
        for copy in copies:
            copy.wait()
        count_ref, type_ref, window_ref, slot_ref, weight_ref, error_ref, value_ref = near
    else:
        if mode == "start":
            recv_ref, slot_ref, weight_ref, error_ref = refs[:4]
            refs = refs[4:]
        else:
            recv_ref, slot_ref, weight_ref, error_ref, value_ref, before_ref = refs[:6]
            refs = refs[6:]
        out_ref, observed_ref, scalar_ref, total, table = refs
    points = slot_ref.shape[0]
    blocks = error_ref.shape[0]
    devices = pack.devices
    wide = points * BLOCK_ROWS
    spare = pack.spare_tile * SUB
    if mode != "right":
        total[...] = jnp.zeros_like(total)
        for j in range(pack.rows):
            table[j] = recv_ref[pl.ds(j, devices, stride=pack.rows), :]
        norm = pack.spare(jnp.sum(table[spare], axis=0, keepdims=True))
        if mode == "start":
            ratio, square = jnp.zeros_like(norm), norm
        else:
            cross = pack.spare(jnp.sum(table[spare + 1], axis=0, keepdims=True))
            ratio = norm / before_ref[0:1, 0:1]
            square = norm + 2.0 * ratio * cross + ratio * ratio * before_ref[2:3, 0:1]
        row = iota((SUB, LANES), 0)
        scalar_ref[...] = jnp.where(row == 0, norm, jnp.where(row == 1, ratio, square))

    ids = iota((LANES, BLOCK_ROWS), 0)

    def row(x):
        return jnp.concatenate([x[k : k + 1, :] for k in range(points)], axis=1)

    def some(first, energy):
        group = [first * together + i for i in range(together)]
        places, picks, owners, weights, values = [], [], [], [], []
        for b in group:
            window = window_ref[b]
            places.append((window >> log2(pack.per)) * SUB + type_ref[b])
            shift = (window & (pack.per - 1)) * pack.slots
            lanes = pl.ds(pl.multiple_of(b * BLOCK_ROWS, BLOCK_ROWS), BLOCK_ROWS)
            slot = slot_ref[:, lanes]
            lane = (slot & (pack.slots - 1)) + shift
            picks.append(
                jnp.concatenate(
                    [jnp.where(ids == lane[k : k + 1, :], 1.0, 0.0) for k in range(points)],
                    axis=1,
                ).astype(BF16)
            )
            owners.append(iota((devices, wide), 0) == row(slot >> pack.group_bits))
            weights.append(row(weight_ref[:, lanes]))
        if mode == "right":
            values = [value_ref[pl.ds(b, 1), :] for b in group]
        else:
            found = []
            for j, pick in zip(places, picks):
                top, rest = halves(table[j])
                found.append(dot(jnp.concatenate([top, rest], axis=0).astype(BF16), pick))
            for b, both, owner, weight in zip(group, found, owners, weights):
                both = both[:devices] + both[devices:]
                both = jnp.sum(jnp.where(owner, both, 0.0), axis=0, keepdims=True) * weight
                value = both[:, :BLOCK_ROWS]
                for k in range(1, points):
                    value = value + both[:, k * BLOCK_ROWS : (k + 1) * BLOCK_ROWS]
                if mode == "next":
                    value = value + ratio * value_ref[pl.ds(b, 1), :]
                values.append(value)
            for b, value in zip(group, values):
                observed_ref[pl.ds(b, 1), :] = value
        sums = []
        for b, pick, owner, weight, value in zip(group, picks, owners, weights, values):
            live = iota((1, BLOCK_ROWS), 1) < count_ref[b]
            weighted = jnp.where(live, error_ref[pl.ds(b, 1), :], 0.0) * value
            energy = energy + weighted * value
            spread = jnp.concatenate([weighted] * points, axis=1) * weight
            top, rest = halves(jnp.where(owner, spread, 0.0))
            sums.append(
                lax.dot_general(
                    jnp.concatenate([top, rest], axis=0).astype(BF16),
                    pick,
                    NT,
                    preferred_element_type=F32,
                )
            )
        for j, both in zip(places, sums):
            total[j] += both[:devices] + both[devices:]
        return energy

    together = 8
    while blocks % together:
        together -= 1
    energy = jnp.zeros((1, BLOCK_ROWS), F32)
    energy = lax.fori_loop(0, blocks // together, some, energy)
    energy = jnp.sum(energy, axis=1, keepdims=True)
    for j in range(pack.rows):
        chunk = total[j]
        if j == spare:
            chunk = jnp.where(pack.group((devices, LANES)) == pack.spare_group, energy, chunk)
        out_ref[pl.ds(j, devices, stride=pack.rows), :] = chunk


def collect_kernel(pack, lat_cells, with_winds, *refs):
    if with_winds:
        recv_ref, send_ref, zonal_ref, merid_ref = refs[:4]
        refs = refs[4:]
    else:
        recv_ref, send_ref = refs[:2]
        refs = refs[2:]
    main_ref, west_ref, east_ref, scalar_ref = refs[:4]
    if with_winds:
        held, near, done = refs[4:-3], refs[-3:-1], refs[-1]
        copies = [
            pltpu.make_async_copy(src, dst, done.at[i])
            for i, (src, dst) in enumerate(zip((zonal_ref, merid_ref), near))
        ]
        for copy in copies:
            copy.start()
    lon_cells = main_ref.shape[2]
    cols = lon_cells // LANES
    tiles = pack.recv // LANES
    send = send_ref[...]
    pick = jnp.where(iota((LANES, pack.recv), 0) == (send & (LANES - 1)), 1.0, 0.0).astype(BF16)
    high = send >> log2(LANES)
    strips = {}

    def note(slab, left, right):
        at = slab * HALO
        q, s = at // LANES, at % LANES
        lane = iota((SUB, LANES), 1)
        inside = (lane >= s) & (lane < s + HALO)
        west, east = strips.get(q, (jnp.zeros((SUB, LANES), F32),) * 2)
        west = jnp.where(inside, turn(left, s), west)
        east = jnp.where(inside, turn(right, s - (LANES - HALO)), east)
        strips[q] = (west, east)

    for w in range(WIN):
        typed = jnp.concatenate([pack.read(recv_ref, w, t) for t in range(tiles)], axis=1)
        masked = []
        for part in halves(typed):
            masked += [
                jnp.where(high == h, part, 0.0) for h in range(lat_cells * cols)
            ]
        both = lax.dot_general(
            jnp.concatenate(masked, axis=0).astype(BF16), pick, NT, preferred_element_type=F32
        )
        count = lat_cells * cols * SUB
        forcing = both[:count] + both[count:]
        for row in range(lat_cells):
            slab = w * lat_cells + row
            pieces = [
                forcing[(row * cols + c) * SUB : (row * cols + c + 1) * SUB] for c in range(cols)
            ]
            for c in range(cols):
                main_ref[slab, :, c * LANES : (c + 1) * LANES] = pieces[c]
            note(slab, pieces[0], pieces[-1])
    if with_winds:
        slab = WIN * lat_cells
        levels = zonal_ref.shape[0] // lat_cells
        for which in range(2):
            copies[which].wait()
            for c in range(cols):
                held[c][...] = near[which][:, c * LANES : (c + 1) * LANES]
            for row in range(lat_cells):
                for part in range(levels // SUB):
                    at = pl.ds(part * SUB * lat_cells + row, SUB, stride=lat_cells)
                    pieces = [held[c][at, :] for c in range(cols)]
                    for c in range(cols):
                        main_ref[slab, :, c * LANES : (c + 1) * LANES] = pieces[c]
                    note(slab, pieces[0], pieces[-1])
                    slab += 1
    for q in range(west_ref.shape[1] // LANES):
        west, east = strips[q]
        west_ref[:, q * LANES : (q + 1) * LANES] = west
        east_ref[:, q * LANES : (q + 1) * LANES] = east
    row = recv_ref[pl.ds(pack.spare_tile * SUB, pack.devices, stride=pack.rows), :]
    energy = pack.spare(jnp.sum(row, axis=0, keepdims=True))
    scalar_ref[...] = jnp.broadcast_to(energy, scalar_ref.shape)


def merge_kernel(halo, lat_cells, main_ref, east_ref, west_ref, up_ref, down_ref):
    slab = 0
    for w, count in enumerate(trims(halo)):
        for row in range(count):
            up_ref[slab] = main_ref[w * lat_cells + lat_cells - count + row]
            down_ref[slab] = main_ref[w * lat_cells + row]
            slab += 1
    for at in range(WIN * lat_cells, main_ref.shape[0]):
        up_ref[slab] = main_ref[at]
        down_ref[slab] = main_ref[at]
        slab += 1
    wide = main_ref.shape[2]
    for ref in (east_ref, west_ref):
        for part in range(ref.shape[1] // wide):
            piece = ref[:, part * wide : (part + 1) * wide]
            up_ref[slab] = piece
            down_ref[slab] = piece
            slab += 1


def model_kernel(pack, mode, dims, edge_ref, *refs):
    layers, levels, lat_cells, lon_cells = dims
    channels = layers * levels
    halo = REACH if mode == "last" else HALO
    rows = lat_cells + 2 * halo
    cols = lon_cells // LANES
    width = lon_cells + LANES
    kept = trims(halo)
    refs = list(refs)

    def take(count):
        got = refs[:count]
        del refs[:count]
        return got

    south_ref, main_ref, north_ref, east_ref, west_ref = take(5)
    into_ref, back_ref = take(2)
    if mode != "right":
        (winds,) = take(1)
        energy_ref, scalar_ref, residual_ref = take(3)
    if mode == "last":
        (energy0_ref, scalar0_ref, first_ref) = take(3)
        increment_out, residual_out = take(2)
    else:
        (send_ref,) = take(1)
        out_ref, state_out = take(2)
        if mode == "right":
            (winds,) = take(1)
        (picked,) = take(1)
    fields = take(2)
    forced, coef = take(2)
    ends = refs

    lane = iota((SUB, LANES), 1)

    slabs = main_ref.shape[0]
    parts = east_ref.shape[1] // LANES
    beyond = [sum(kept) + slabs - WIN * lat_cells + i * (parts // cols) for i in range(2)]

    def assemble(slab, block, at):
        q, s = slab * HALO // LANES, slab * HALO % LANES
        if block == 1:
            main = main_ref[slab]
            east, west = (ref[:, q * LANES : (q + 1) * LANES] for ref in (east_ref, west_ref))
        else:
            ref = south_ref if block == 0 else north_ref
            main = ref[at]
            lanes = slice(q % cols * LANES, (q % cols + 1) * LANES)
            east, west = (ref[b + q // cols, :, lanes] for b in beyond)
        right = turn(east, -s)
        left = turn(west, LANES - HALO - s)
        edge = jnp.where(lane < HALO, right, jnp.where(lane >= LANES - HALO, left, 0.0))
        return jnp.concatenate([main, edge], axis=1)

    def source(e):
        at = e - halo
        if at < 0:
            return 0, lat_cells + at
        if at < lat_cells:
            return 1, at
        return 2, at - lat_cells

    for w in range(WIN):
        trim = halo - kept[w] if kept[w] else halo
        for e in range(trim, rows - trim):
            block, row = source(e)
            at = sum(kept[:w]) + (row - (lat_cells - kept[w]) if block == 0 else row)
            forced[w, e] = assemble(w * lat_cells + row, block, at)
    if mode == "right":
        for which in range(2):
            for e in range(rows):
                block, row = source(e)
                for part in range(levels // SUB):
                    at = (which * lat_cells + row) * (levels // SUB) + part
                    winds[which, e, part * SUB : (part + 1) * SUB, :] = assemble(
                        WIN * lat_cells + at, block, sum(kept) + at
                    )

    def prepare(e, carry):
        u, v = winds[0, e + HALO - halo], winds[1, e + HALO - halo]
        coef[0, e] = 1.0 - jnp.abs(u) - jnp.abs(v)
        coef[1, e] = jnp.maximum(u, 0.0)
        coef[2, e] = jnp.maximum(-u, 0.0)
        coef[3, e] = jnp.maximum(v, 0.0)
        coef[4, e] = jnp.maximum(-v, 0.0)
        return carry

    loop(0, rows, 4, prepare)

    into = into_ref[...]
    top, rest = halves(into)
    into = jnp.where(iota(into.shape, 1) < 2 * SUB, top, rest).astype(BF16)

    def force(w, e):
        top, rest = halves(forced[w, e])
        return dot(into, jnp.concatenate([top, rest, top, rest], axis=0).astype(BF16))

    def pieces(part):
        level = slice(part * SUB, (part + 1) * SUB)
        return level, [
            slice(v * levels + part * SUB, v * levels + (part + 1) * SUB) for v in range(layers)
        ]

    def adjoint(field, e, put, extra=None):
        for part in range(levels // SUB):
            level, chans = pieces(part)
            keep, west, east = coef[0, e, level], coef[1, e, level], coef[2, e, level]
            south, north = coef[3, e + 1, level], coef[4, e - 1, level]
            for chan in chans:
                here = field[e, chan]
                result = (
                    keep * here
                    + turn(west * here, -1)
                    + turn(east * here, 1)
                    + south * field[e + 1, chan]
                    + north * field[e - 1, chan]
                )
                if extra is not None:
                    result = result + extra[chan]
                put(chan, result)

    def tangent(field, e, put):
        for part in range(levels // SUB):
            level, chans = pieces(part)
            keep, west, east = coef[0, e, level], coef[1, e, level], coef[2, e, level]
            south, north = coef[3, e, level], coef[4, e, level]
            for chan in chans:
                here = field[e, chan]
                put(
                    chan,
                    keep * here
                    + west * turn(here, 1)
                    + east * turn(here, -1)
                    + south * field[e - 1, chan]
                    + north * field[e + 1, chan],
                )

    def put_in(field, e):
        def put(chan, value):
            field[e, chan] = value

        return put

    def begin(e, carry):
        fields[0][e] = force(WIN - 1, e)
        return carry

    loop(0, rows, 8, begin)
    now = 0
    for step in range(1, REACH):
        old, new = fields[now], fields[1 - now]
        w = WIN - 1 - step // STEP_WIN if step % STEP_WIN == 0 else None

        def body(e, carry, old=old, new=new, w=w):
            extra = None if w is None else force(w, e)
            adjoint(old, e, put_in(new, e), extra)
            return carry

        loop(step, rows - step, 4 if w is not None else 2, body)
        now = 1 - now
    old, new = fields[now], fields[1 - now]

    if mode != "right":
        alpha = scalar_ref[0:1, 0:1] / (scalar_ref[2:3, 0:1] + energy_ref[0:1, 0:1])
        ratio = scalar_ref[1:2, 0:1]
    if mode == "last":
        alpha0 = scalar0_ref[0:1, 0:1] / (scalar0_ref[2:3, 0:1] + energy0_ref[0:1, 0:1])

        def finish(row, carry):
            e = row + halo

            def put(chan, value):
                at = pl.ds(chan.start * lat_cells + row, SUB, stride=lat_cells)
                for c in range(cols):
                    part = slice(c * LANES, (c + 1) * LANES)
                    residual = residual_ref[row + REACH, chan, part]
                    first = first_ref[row + REACH, chan, part]
                    direction = residual + ratio * first
                    image = direction + value[:, part]
                    ends[c][at, :] = alpha0 * first + alpha * direction
                    ends[cols + c][at, :] = residual - alpha * image

            adjoint(old, e, put, force(0, e))
            return carry

        loop(0, lat_cells, 4, finish)
        for c in range(cols):
            part = slice(c * LANES, (c + 1) * LANES)
            increment_out[:, part] = ends[c][...]
            residual_out[:, part] = ends[cols + c][...]
        return

    def update(e, sums):
        valid = jnp.where(e < HALO, edge_ref[0], jnp.where(e >= HALO + lat_cells, edge_ref[1], 1))
        scale = valid.astype(F32)
        inside = jnp.where((e >= HALO) & (e < HALO + lat_cells), 1, 0).astype(F32)
        at = e - REACH
        sums = list(sums)

        def put(chan, value):
            value = value * scale
            if mode != "right":
                before = residual_ref[at, chan]
                value = before - alpha * (before + value)
            state_out[at, chan] = value
            new[e, chan] = value
            kept = value[:, :lon_cells] * inside
            sums[0] = sums[0] + kept * value[:, :lon_cells]
            if mode != "right":
                sums[1] = sums[1] + kept * before[:, :lon_cells]

        adjoint(old, e, put, force(0, e))
        return tuple(sums)

    zero = jnp.zeros((SUB, lon_cells), F32)
    sums = (zero,) if mode == "right" else (zero, zero)
    sums = loop(REACH, rows - REACH, 4, update, sums)
    sums = [jnp.sum(jnp.sum(s, axis=1, keepdims=True), axis=0, keepdims=True) for s in sums]
    now = 1 - now

    back = back_ref[...]
    top, rest = halves(back)
    back = jnp.where(iota(back.shape, 0) < SUB, top, rest).astype(BF16)

    def look(field, w):
        def body(row, carry):
            top, rest = halves(field[row + HALO, :, :lon_cells])
            both = dot(back, jnp.concatenate([top, rest], axis=0).astype(BF16))
            typed = both[:SUB] + both[SUB:]
            for c in range(cols):
                at = pl.multiple_of(((w * lat_cells + row) * cols + c) * SUB, SUB)
                picked[pl.ds(at, SUB), :] = typed[:, c * LANES : (c + 1) * LANES]
            return carry

        loop(0, lat_cells, 8, body)

    look(fields[now], 0)
    for step in range(1, REACH + 1):
        old, new = fields[now], fields[1 - now]

        def body(e, carry, old=old, new=new):
            tangent(old, e, put_in(new, e))
            return carry

        loop(REACH + step, rows - REACH - step, 2, body)
        now = 1 - now
        if step % STEP_WIN == 0:
            look(fields[now], step // STEP_WIN)

    row = iota((SUB, LANES), 0)
    spare = jnp.where(row == 0, sums[0], 0.0)
    if mode != "right":
        spare = jnp.where(row == 1, sums[1], spare)
    top, rest = halves(picked[...])
    values = jnp.concatenate([top, rest], axis=1).astype(BF16)
    chunk = 2 * LANES
    parts = lat_cells * cols
    for c in range(pack.recv // chunk):
        send = send_ref[:, c * chunk : (c + 1) * chunk]
        pick = jnp.where(iota((LANES, chunk), 0) == (send & (LANES - 1)), 1.0, 0.0)
        pick = jnp.concatenate([pick, pick], axis=0).astype(BF16)
        high = send >> log2(LANES)
        every = dot(values, pick)
        typed = []
        for w in range(WIN):
            found = jnp.zeros((SUB, chunk), F32)
            for h in range(parts):
                at = (w * parts + h) * SUB
                found = jnp.where(high == h, every[at : at + SUB], found)
            typed.append(found)
        for t in range(chunk // LANES):
            lanes = slice(t * LANES, (t + 1) * LANES)
            pack.write(out_ref, [x[:, lanes] for x in typed], spare, c * (chunk // LANES) + t)


def call(kernel, out_shapes, args, places, scratch, limit=40):
    specs = [pl.BlockSpec(memory_space=place) for place in places]
    specs += [pl.BlockSpec(memory_space=pltpu.VMEM)] * (len(args) - len(places))
    return pl.pallas_call(
        kernel,
        out_shape=[jax.ShapeDtypeStruct(s, F32) for s in out_shapes],
        in_specs=specs,
        out_specs=[pl.BlockSpec(memory_space=pltpu.VMEM)] * len(out_shapes),
        scratch_shapes=[pltpu.VMEM(s, F32) if isinstance(s, tuple) else s for s in scratch],
        compiler_params=pltpu.CompilerParams(vmem_limit_bytes=limit << 20),
    )(*args)


def shards(
    zonal_wind,
    merid_wind,
    operator_rows,
    innovation,
    error_weight,
    interp_weight,
    obs_slot,
    block_count,
    block_type,
    block_window,
    send_cols,
):
    levels, lat_cells, lon_cells = zonal_wind.shape
    types, channels = operator_rows.shape
    layers = channels // levels
    n_lat, n_lon = lax.axis_size("lat"), lax.axis_size("lon")
    recv = send_cols.shape[1]
    blocks = block_count.shape[0]
    pack = Packing(n_lat * n_lon, recv)
    assert types == SUB and lat_cells >= HALO and lon_cells % LANES == 0
    dims = (layers, levels, lat_cells, lon_cells)
    width = lon_cells + LANES
    chunks = (pack.devices * pack.rows, LANES)
    block_args = [block_count, block_type, block_window]
    rows_of = lambda x: x.reshape(blocks, BLOCK_ROWS)
    error = rows_of(error_weight)
    total = (pack.rows, pack.devices, LANES)
    band = lax.axis_index("lat")
    edges = jnp.stack([band > 0, band < n_lat - 1]).astype(jnp.int32)
    into = jnp.tile(operator_rows.T, (1, 4))
    back = jnp.tile(operator_rows, (2, 2))

    def exchange(x):
        x = x.reshape(pack.devices, pack.rows, LANES)
        x = lax.all_to_all(x, AXES, split_axis=0, concat_axis=0, tiled=True)
        return x.reshape(chunks)

    def send(x, up, right):
        pairs = [
            (i * n_lon + j, (i + up) * n_lon + (j + right) % n_lon)
            for i in range(n_lat)
            for j in range(n_lon)
            if 0 <= i + up < n_lat
        ]
        return lax.ppermute(x, AXES, pairs)

    def collect(received, with_winds, halo):
        slabs = WIN * lat_cells
        args, places, scratch = [received, send_cols], [], []
        if with_winds:
            slabs += 2 * lat_cells * (levels // SUB)
            winds2d = (levels * lat_cells, lon_cells)
            args += [x.reshape(winds2d) for x in (zonal_wind, merid_wind)]
            places = [pltpu.VMEM, pltpu.VMEM, pl.ANY, pl.ANY]
            scratch = [(winds2d[0], LANES)] * (lon_cells // LANES)
            scratch += [winds2d, winds2d, pltpu.SemaphoreType.DMA((2,))]
        strip = (SUB, -(-slabs * HALO // lon_cells) * lon_cells)
        main, west, east, energy = call(
            functools.partial(collect_kernel, pack, lat_cells, with_winds),
            [(slabs, SUB, lon_cells), strip, strip, (SUB, LANES)],
            args,
            places,
            scratch,
            48 if with_winds else 40,
        )
        east, west = send(west, 0, -1), send(east, 0, 1)
        count = sum(trims(halo)) + slabs - WIN * lat_cells + 2 * strip[1] // lon_cells
        up, down = call(
            functools.partial(merge_kernel, halo, lat_cells),
            [(count, SUB, lon_cells)] * 2,
            [main, east, west],
            [],
            [],
        )
        return [send(up, 1, 0), main, send(down, -1, 0), east, west], energy

    def model(mode, halos, extra):
        ends = (channels * lat_cells, lon_cells)
        state = (lat_cells + 2 * REACH, channels, width)
        rows = lat_cells + 2 * (REACH if mode == "last" else HALO)
        outs = [ends, ends] if mode == "last" else [chunks, state]
        scratch = [(rows, channels, width)] * 2
        scratch += [(WIN, rows, SUB, width), (5, rows, levels, width)]
        if mode == "right":
            outs += [(2, rows, levels, width)]
        if mode == "last":
            scratch += [(ends[0], LANES)] * (2 * lon_cells // LANES)
        if mode != "last":
            scratch = [(WIN * lat_cells * lon_cells // LANES * SUB, LANES)] + scratch
        return call(
            functools.partial(model_kernel, pack, mode, dims),
            outs,
            [edges, *halos, into, back, *extra],
            [pltpu.SMEM],
            scratch,
        )

    def observe(mode, received, extra):
        outs, scratch = [chunks], [total]
        args = block_args + received + [obs_slot, interp_weight, error] + extra
        if mode == "right":
            places, limit = [pl.ANY] * len(args), 56
            scratch += [pltpu.SMEM(x.shape, x.dtype) for x in args[:3]]
            scratch += [pltpu.VMEM(x.shape, x.dtype) for x in args[3:]]
            scratch += [pltpu.SemaphoreType.DMA((len(args),))]
        else:
            places, limit = [pltpu.SMEM] * 3, 40
            outs += [(blocks, BLOCK_ROWS), (SUB, LANES)]
            scratch += [total]
        kernel = functools.partial(observe_kernel, pack, mode)
        return call(kernel, outs, args, places, scratch, limit)

    assert ITERS == 2
    (chunk,) = observe("right", [], [rows_of(innovation)])
    halos, _ = collect(exchange(chunk), True, HALO)
    chunk, right, winds = model("right", halos, [send_cols])
    chunk, seen, scalar0 = observe("start", [exchange(chunk)], [])
    halos, energy0 = collect(exchange(chunk), False, HALO)
    chunk, residual = model("next", halos, [winds, energy0, scalar0, right, send_cols])
    chunk, seen, scalar1 = observe("next", [exchange(chunk)], [seen, scalar0])
    halos, energy1 = collect(exchange(chunk), False, REACH)
    ends = model(
        "last", halos, [winds, energy1, scalar1, residual, energy0, scalar0, right]
    )
    return tuple(x.reshape(layers, levels, lat_cells, lon_cells) for x in ends)


def solution(mesh):
    return jax.shard_map(
        shards,
        mesh=mesh,
        in_specs=(
            P(None, "lat", "lon"),
            P(None, "lat", "lon"),
            P(),
            P(("lat", "lon")),
            P(("lat", "lon")),
            P(None, ("lat", "lon")),
            P(None, ("lat", "lon")),
            P(("lat", "lon")),
            P(("lat", "lon")),
            P(("lat", "lon")),
            P(("lat", "lon"), None),
        ),
        out_specs=(P(None, None, "lat", "lon"), P(None, None, "lat", "lon")),
        check_vma=False,
    )
```

```python
import functools

import jax
import jax.numpy as jnp
from jax import lax
from jax.experimental import pallas as pl
from jax.experimental.pallas import tpu as pltpu
from jax.sharding import PartitionSpec as P

WIN = 3
STEP_WIN = 2
ITERS = 2
BLOCK_ROWS = 128
LANES = 128
SUB = 8
REACH = STEP_WIN * (WIN - 1)
HALO = 2 * REACH
AXES = ("lat", "lon")
F32 = jnp.float32
BF16 = jnp.bfloat16
NT = (((1,), (1,)), ((), ()))


def log2(n):
    assert n & (n - 1) == 0
    return n.bit_length() - 1


def iota(shape, dim):
    return lax.broadcasted_iota(jnp.int32, shape, dim)


def halves(x):
    top = x.astype(BF16).astype(F32)
    return top, x - top


def dot(a, b):
    return jnp.dot(a, b, preferred_element_type=F32)


def loop(low, high, step, body, carry=0):
    count = high - low
    while count % step:
        step -= 1

    def some(i, carry):
        for k in range(step):
            carry = body(low + i * step + k, carry)
        return carry

    return lax.fori_loop(0, count // step, some, carry)


def trims(halo):
    return [max(halo - STEP_WIN * (WIN - 1 - w), 0) for w in range(WIN)]


class Packing:
    def __init__(self, devices, recv):
        self.devices = devices
        self.recv = recv
        self.slots = recv // devices
        assert self.slots <= LANES and recv % LANES == 0
        self.per = LANES // self.slots
        self.full = WIN // self.per
        self.left = WIN - self.full * self.per
        self.short = -(-self.left * SUB // self.per)
        self.spare = self.full * SUB + self.short
        self.rows = self.spare + 1
        self.group_bits = log2(self.slots)

    def group(self, shape):
        return iota(shape, len(shape) - 1) >> self.group_bits

    def place(self, window, kind):
        row = (window >> log2(self.per)) * SUB + kind
        group = window & (self.per - 1)
        if self.left:
            at = (window - self.full * self.per) * SUB + kind
            late = window >= self.full * self.per
            row = jnp.where(late, self.full * SUB + lax.rem(at, self.short), row)
            group = jnp.where(late, lax.div(at, self.short), group)
        return row, group * self.slots

    def sums(self, row):
        total = jnp.sum(row, axis=0, keepdims=True)
        lane = iota(total.shape, 1)
        return [
            jnp.sum(jnp.where(lane == at, total, 0.0), axis=1, keepdims=True)
            for at in (0, LANES // 2)
        ]

    def write(self, out_ref, typed, spare, tile):
        late = typed[self.full * self.per :]
        late = late[0] if len(late) == 1 else jnp.concatenate(late, axis=0)
        for d in range(self.per):
            base = (tile * self.per + d) * self.rows
            for part in range(self.full):
                chunk = None
                for g in range(self.per):
                    piece = turn(typed[part * self.per + g], (g - d) * self.slots)
                    chunk = piece if g == 0 else self.select(g, piece, chunk)
                out_ref[base + part * SUB : base + (part + 1) * SUB, :] = chunk
            chunk = jnp.zeros((self.short, LANES), F32)
            for g in range(self.per):
                piece = turn(late, (g - d) * self.slots)
                piece = piece[g * self.short : (g + 1) * self.short]
                chunk = piece if g == 0 else self.select(g, piece, chunk)
            base += self.full * SUB
            out_ref[base : base + self.short, :] = chunk
            out_ref[base + self.short : base + self.short + 1, :] = spare

    def select(self, group, yes, no):
        return jnp.where(self.group(yes.shape) == group, yes, no)

    def read(self, ref, tile):
        typed = [None] * WIN
        for d in range(self.per):
            base = (tile * self.per + d) * self.rows
            for part in range(self.full):
                piece = ref[base + part * SUB : base + (part + 1) * SUB, :]
                for g in range(self.per):
                    w = part * self.per + g
                    found = turn(piece, (d - g) * self.slots)
                    typed[w] = found if d == 0 else self.select(d, found, typed[w])
            base += self.full * SUB
            piece = ref[base : base + self.short, :]
            late = [turn(piece, (d - g) * self.slots) for g in range(self.per)]
            late = jnp.concatenate(late, axis=0)
            for i in range(self.left):
                w = self.full * self.per + i
                found = late[i * SUB : (i + 1) * SUB]
                typed[w] = found if d == 0 else self.select(d, found, typed[w])
        return typed


def turn(x, shift):
    shift %= x.shape[-1]
    return pltpu.roll(x, shift, len(x.shape) - 1) if shift else x


def note(strips, slab, left, right):
    q, s = slab * HALO // LANES, slab * HALO % LANES
    lane = iota((SUB, LANES), 1)
    inside = (lane >= s) & (lane < s + HALO)
    west, east = strips.get(q, (jnp.zeros((SUB, LANES), F32),) * 2)
    west = jnp.where(inside, turn(left, s), west)
    east = jnp.where(inside, turn(right, s - (LANES - HALO)), east)
    strips[q] = (west, east)


def lay_winds(first, refs, held, out_ref):
    cols, lat_cells = len(held), first // WIN
    slab, strips = 0, {}
    for ref in refs:
        for c in range(cols):
            held[c][...] = ref[:, c * LANES : (c + 1) * LANES]
        for row in range(lat_cells):
            for part in range(ref.shape[0] // lat_cells // SUB):
                at = pl.ds(part * SUB * lat_cells + row, SUB, stride=lat_cells)
                pieces = [held[c][at, :] for c in range(cols)]
                for c in range(cols):
                    out_ref[slab, :, c * LANES : (c + 1) * LANES] = pieces[c]
                note(strips, first + slab, pieces[0], pieces[-1])
                slab += 1
    count = (out_ref.shape[0] - 1 - slab) // 2
    for q in range(count * cols):
        for side in range(2):
            piece = strips[q][side] if q in strips else jnp.zeros((SUB, LANES), F32)
            lanes = slice(q % cols * LANES, (q % cols + 1) * LANES)
            out_ref[slab + side * count + q // cols, :, lanes] = piece


def observe_kernel(pack, mode, lat_cells, count_ref, type_ref, window_ref, *refs):
    if mode == "right":
        far = (count_ref, type_ref, window_ref) + refs[:7]
        out_ref, winds_ref, total = refs[7:10]
        near, held, done = refs[10:20], refs[20:-1], refs[-1]
        copies = [
            pltpu.make_async_copy(src, dst, done.at[i])
            for i, (src, dst) in enumerate(zip(far, near))
        ]
        for copy in copies:
            copy.start()
        total[...] = jnp.zeros_like(total)
        for copy in copies[:7]:
            copy.wait()
        count_ref, type_ref, window_ref, slot_ref, weight_ref, error_ref, value_ref = near[:7]
    else:
        if mode == "start":
            recv_ref, slot_ref, weight_ref, error_ref = refs[:4]
            refs = refs[4:]
        else:
            recv_ref, slot_ref, weight_ref, error_ref, value_ref, before_ref = refs[:6]
            refs = refs[6:]
        out_ref, observed_ref, scalar_ref, total, table = refs
    points = slot_ref.shape[0]
    blocks = error_ref.shape[0]
    devices = pack.devices
    wide = points * BLOCK_ROWS
    if mode != "right":
        total[...] = jnp.zeros_like(total)
        for j in range(pack.rows):
            table[j] = recv_ref[pl.ds(j, devices, stride=pack.rows), :]
        norm, cross = pack.sums(table[pack.spare])
        if mode == "start":
            ratio, square = jnp.zeros_like(norm), norm
        else:
            ratio = norm / before_ref[0:1, 0:1]
            square = norm + 2.0 * ratio * cross + ratio * ratio * before_ref[2:3, 0:1]
        row = iota((SUB, LANES), 0)
        scalar_ref[...] = jnp.where(row == 0, norm, jnp.where(row == 1, ratio, square))

    ids = iota((LANES, BLOCK_ROWS), 0)

    def row(x):
        return jnp.concatenate([x[k : k + 1, :] for k in range(points)], axis=1)

    def some(first, energy):
        group = [first * together + i for i in range(together)]
        places, picks, owners, weights, values = [], [], [], [], []
        for b in group:
            place, shift = pack.place(window_ref[b], type_ref[b])
            places.append(place)
            lanes = pl.ds(pl.multiple_of(b * BLOCK_ROWS, BLOCK_ROWS), BLOCK_ROWS)
            slot = slot_ref[:, lanes]
            lane = (slot & (pack.slots - 1)) + shift
            picks.append(
                jnp.concatenate(
                    [jnp.where(ids == lane[k : k + 1, :], 1.0, 0.0) for k in range(points)],
                    axis=1,
                ).astype(BF16)
            )
            owners.append(iota((devices, wide), 0) == row(slot >> pack.group_bits))
            weights.append(row(weight_ref[:, lanes]))
        if mode == "right":
            values = [value_ref[pl.ds(b, 1), :] for b in group]
        else:
            found = []
            for j, pick in zip(places, picks):
                top, rest = halves(table[j])
                found.append(dot(jnp.concatenate([top, rest], axis=0).astype(BF16), pick))
            for b, both, owner, weight in zip(group, found, owners, weights):
                both = both[:devices] + both[devices:]
                both = jnp.sum(jnp.where(owner, both, 0.0), axis=0, keepdims=True) * weight
                value = both[:, :BLOCK_ROWS]
                for k in range(1, points):
                    value = value + both[:, k * BLOCK_ROWS : (k + 1) * BLOCK_ROWS]
                if mode == "next":
                    value = value + ratio * value_ref[pl.ds(b, 1), :]
                values.append(value)
            for b, value in zip(group, values):
                observed_ref[pl.ds(b, 1), :] = value
        sums = []
        for b, pick, owner, weight, value in zip(group, picks, owners, weights, values):
            live = iota((1, BLOCK_ROWS), 1) < count_ref[b]
            weighted = jnp.where(live, error_ref[pl.ds(b, 1), :], 0.0) * value
            energy = energy + weighted * value
            spread = jnp.concatenate([weighted] * points, axis=1) * weight
            top, rest = halves(jnp.where(owner, spread, 0.0))
            sums.append(
                lax.dot_general(
                    jnp.concatenate([top, rest], axis=0).astype(BF16),
                    pick,
                    NT,
                    preferred_element_type=F32,
                )
            )
        for j, both in zip(places, sums):
            total[j] += both[:devices] + both[devices:]
        return energy

    together = 8
    while blocks % together:
        together -= 1
    energy = jnp.zeros((1, BLOCK_ROWS), F32)
    energy = lax.fori_loop(0, blocks // together, some, energy)
    energy = jnp.sum(energy, axis=1, keepdims=True)
    for j in range(pack.rows):
        chunk = total[j]
        if j == pack.spare:
            chunk = jnp.broadcast_to(energy, (devices, LANES))
        out_ref[pl.ds(j, devices, stride=pack.rows), :] = chunk
    if mode == "right":
        for copy in copies[7:]:
            copy.wait()
        lay_winds(WIN * lat_cells, near[7:9], held, winds_ref)
        wide = winds_ref.shape[2]
        send = near[9][...].astype(F32)
        rows = [send[:, i * wide : (i + 1) * wide] for i in range(pack.recv // wide)]
        rows += [jnp.zeros((1, wide), F32)] * (SUB - len(rows))
        winds_ref[winds_ref.shape[0] - 1] = jnp.concatenate(rows, axis=0)


def collect_kernel(pack, lat_cells, with_winds, recv_ref, send_ref, *refs):
    main_ref, west_ref, east_ref, scalar_ref = refs
    lon_cells = main_ref.shape[2]
    cols = lon_cells // LANES
    tiles = pack.recv // LANES
    strips = {}
    if with_winds:
        send = send_ref[send_ref.shape[0] - 1]
        send = [send[i : i + 1] for i in range(pack.recv // lon_cells)]
        send = jnp.concatenate(send, axis=1).astype(jnp.int32)
        count = main_ref.shape[0] - WIN * lat_cells
        main_ref[WIN * lat_cells :] = send_ref[:count]
        half = west_ref.shape[1] // lon_cells
        for q in range(half * cols):
            lanes = slice(q % cols * LANES, (q % cols + 1) * LANES)
            at = count + q // cols
            strips[q] = (send_ref[at, :, lanes], send_ref[at + half, :, lanes])
    else:
        send = send_ref[...]
    pick = jnp.where(iota((LANES, pack.recv), 0) == (send & (LANES - 1)), 1.0, 0.0).astype(BF16)
    high = send >> log2(LANES)

    every = [pack.read(recv_ref, t) for t in range(tiles)]
    for w in range(WIN):
        typed = jnp.concatenate([x[w] for x in every], axis=1)
        masked = []
        for part in halves(typed):
            masked += [
                jnp.where(high == h, part, 0.0) for h in range(lat_cells * cols)
            ]
        both = lax.dot_general(
            jnp.concatenate(masked, axis=0).astype(BF16), pick, NT, preferred_element_type=F32
        )
        count = lat_cells * cols * SUB
        forcing = both[:count] + both[count:]
        for row in range(lat_cells):
            slab = w * lat_cells + row
            pieces = [
                forcing[(row * cols + c) * SUB : (row * cols + c + 1) * SUB] for c in range(cols)
            ]
            for c in range(cols):
                main_ref[slab, :, c * LANES : (c + 1) * LANES] = pieces[c]
            note(strips, slab, pieces[0], pieces[-1])
    for q in range(west_ref.shape[1] // LANES):
        west, east = strips[q]
        west_ref[:, q * LANES : (q + 1) * LANES] = west
        east_ref[:, q * LANES : (q + 1) * LANES] = east
    energy, _ = pack.sums(recv_ref[pl.ds(pack.spare, pack.devices, stride=pack.rows), :])
    scalar_ref[...] = jnp.broadcast_to(energy, scalar_ref.shape)


def merge_kernel(halo, lat_cells, main_ref, east_ref, west_ref, up_ref, down_ref):
    slab = 0
    for w, count in enumerate(trims(halo)):
        for row in range(count):
            up_ref[slab] = main_ref[w * lat_cells + lat_cells - count + row]
            down_ref[slab] = main_ref[w * lat_cells + row]
            slab += 1
    for at in range(WIN * lat_cells, main_ref.shape[0]):
        up_ref[slab] = main_ref[at]
        down_ref[slab] = main_ref[at]
        slab += 1
    wide = main_ref.shape[2]
    for ref in (east_ref, west_ref):
        for part in range(ref.shape[1] // wide):
            piece = ref[:, part * wide : (part + 1) * wide]
            up_ref[slab] = piece
            down_ref[slab] = piece
            slab += 1


def model_kernel(pack, mode, dims, edge_ref, *refs):
    layers, levels, lat_cells, lon_cells = dims
    channels = layers * levels
    halo = REACH if mode == "last" else HALO
    rows = lat_cells + 2 * halo
    cols = lon_cells // LANES
    width = lon_cells + LANES
    kept = trims(halo)
    refs = list(refs)

    def take(count):
        got = refs[:count]
        del refs[:count]
        return got

    south_ref, main_ref, north_ref, east_ref, west_ref = take(5)
    into_ref, back_ref = take(2)
    if mode != "right":
        (winds,) = take(1)
        energy_ref, scalar_ref, residual_ref = take(3)
    if mode == "last":
        (energy0_ref, scalar0_ref, first_ref) = take(3)
        increment_out, residual_out = take(2)
    else:
        (send_ref,) = take(1)
        out_ref, state_out = take(2)
        if mode == "right":
            (winds,) = take(1)
        (picked,) = take(1)
    fields = take(2)
    forced, coef = take(2)
    ends = refs

    lane = iota((SUB, LANES), 1)

    slabs = main_ref.shape[0]
    parts = east_ref.shape[1] // LANES
    beyond = [sum(kept) + slabs - WIN * lat_cells + i * (parts // cols) for i in range(2)]

    def assemble(slab, block, at):
        q, s = slab * HALO // LANES, slab * HALO % LANES
        if block == 1:
            main = main_ref[slab]
            east, west = (ref[:, q * LANES : (q + 1) * LANES] for ref in (east_ref, west_ref))
        else:
            ref = south_ref if block == 0 else north_ref
            main = ref[at]
            lanes = slice(q % cols * LANES, (q % cols + 1) * LANES)
            east, west = (ref[b + q // cols, :, lanes] for b in beyond)
        right = turn(east, -s)
        left = turn(west, LANES - HALO - s)
        edge = jnp.where(lane < HALO, right, jnp.where(lane >= LANES - HALO, left, 0.0))
        return jnp.concatenate([main, edge], axis=1)

    def source(e):
        at = e - halo
        if at < 0:
            return 0, lat_cells + at
        if at < lat_cells:
            return 1, at
        return 2, at - lat_cells

    for w in range(WIN):
        trim = halo - kept[w] if kept[w] else halo
        for e in range(trim, rows - trim):
            block, row = source(e)
            at = sum(kept[:w]) + (row - (lat_cells - kept[w]) if block == 0 else row)
            forced[w, e] = assemble(w * lat_cells + row, block, at)
    if mode == "right":
        for which in range(2):
            for e in range(rows):
                block, row = source(e)
                for part in range(levels // SUB):
                    at = (which * lat_cells + row) * (levels // SUB) + part
                    wind = assemble(WIN * lat_cells + at, block, sum(kept) + at)
                    if block != 1:
                        wind = jnp.where(edge_ref[block // 2] > 0, wind, 0.0)
                    winds[which, e, part * SUB : (part + 1) * SUB, :] = wind

    def prepare(e, carry):
        u, v = winds[0, e + HALO - halo], winds[1, e + HALO - halo]
        coef[0, e] = 1.0 - jnp.abs(u) - jnp.abs(v)
        coef[1, e] = jnp.maximum(u, 0.0)
        coef[2, e] = jnp.maximum(-u, 0.0)
        coef[3, e] = jnp.maximum(v, 0.0)
        coef[4, e] = jnp.maximum(-v, 0.0)
        return carry

    loop(0, rows, 4, prepare)

    into = into_ref[...]
    top, rest = halves(into)
    into = jnp.where(iota(into.shape, 1) < 2 * SUB, top, rest).astype(BF16)

    def force(w, e):
        top, rest = halves(forced[w, e])
        return dot(into, jnp.concatenate([top, rest, top, rest], axis=0).astype(BF16))

    def pieces(part):
        level = slice(part * SUB, (part + 1) * SUB)
        return level, [
            slice(v * levels + part * SUB, v * levels + (part + 1) * SUB) for v in range(layers)
        ]

    def adjoint(field, e, put, extra=None):
        for part in range(levels // SUB):
            level, chans = pieces(part)
            keep, west, east = coef[0, e, level], coef[1, e, level], coef[2, e, level]
            south, north = coef[3, e + 1, level], coef[4, e - 1, level]
            for chan in chans:
                here = field[e, chan]
                result = (
                    keep * here
                    + turn(west * here, -1)
                    + turn(east * here, 1)
                    + south * field[e + 1, chan]
                    + north * field[e - 1, chan]
                )
                if extra is not None:
                    result = result + extra[chan]
                put(chan, result)

    def tangent(field, e, put):
        for part in range(levels // SUB):
            level, chans = pieces(part)
            keep, west, east = coef[0, e, level], coef[1, e, level], coef[2, e, level]
            south, north = coef[3, e, level], coef[4, e, level]
            for chan in chans:
                here = field[e, chan]
                put(
                    chan,
                    keep * here
                    + west * turn(here, 1)
                    + east * turn(here, -1)
                    + south * field[e - 1, chan]
                    + north * field[e + 1, chan],
                )

    def put_in(field, e):
        def put(chan, value):
            field[e, chan] = value

        return put

    def begin(e, carry):
        fields[0][e] = force(WIN - 1, e)
        return carry

    loop(0, rows, 8, begin)
    now = 0
    for step in range(1, REACH):
        old, new = fields[now], fields[1 - now]
        w = WIN - 1 - step // STEP_WIN if step % STEP_WIN == 0 else None

        def body(e, carry, old=old, new=new, w=w):
            extra = None if w is None else force(w, e)
            adjoint(old, e, put_in(new, e), extra)
            return carry

        loop(step, rows - step, 4 if w is not None else 2, body)
        now = 1 - now
    old, new = fields[now], fields[1 - now]

    if mode != "right":
        alpha = scalar_ref[0:1, 0:1] / (scalar_ref[2:3, 0:1] + energy_ref[0:1, 0:1])
        ratio = scalar_ref[1:2, 0:1]
    if mode == "last":
        alpha0 = scalar0_ref[0:1, 0:1] / (scalar0_ref[2:3, 0:1] + energy0_ref[0:1, 0:1])

        def finish(e, carry):
            row = e - halo

            def put(chan, value):
                at = pl.ds(chan.start * lat_cells + row, SUB, stride=lat_cells)
                for c in range(cols):
                    part = slice(c * LANES, (c + 1) * LANES)
                    residual = residual_ref[row + REACH, chan, part]
                    first = first_ref[row + REACH, chan, part]
                    direction = residual + ratio * first
                    image = direction + value[:, part]
                    ends[c][at, :] = alpha0 * first + alpha * direction
                    ends[cols + c][at, :] = residual - alpha * image

            adjoint(old, e, put, force(0, e))
            return carry

        loop(halo, halo + lat_cells, 4, finish)
        for c in range(cols):
            part = slice(c * LANES, (c + 1) * LANES)
            increment_out[:, part] = ends[c][...]
            residual_out[:, part] = ends[cols + c][...]
        return

    def update(e, sums):
        valid = jnp.where(e < HALO, edge_ref[0], jnp.where(e >= HALO + lat_cells, edge_ref[1], 1))
        scale = valid.astype(F32)
        inside = jnp.where((e >= HALO) & (e < HALO + lat_cells), 1, 0).astype(F32)
        at = e - REACH
        sums = list(sums)

        def put(chan, value):
            value = value * scale
            if mode != "right":
                before = residual_ref[at, chan]
                value = before - alpha * (before + value)
            state_out[at, chan] = value
            new[e, chan] = value
            kept = value[:, :lon_cells] * inside
            sums[0] = sums[0] + kept * value[:, :lon_cells]
            if mode != "right":
                sums[1] = sums[1] + kept * before[:, :lon_cells]

        adjoint(old, e, put, force(0, e))
        return tuple(sums)

    zero = jnp.zeros((SUB, lon_cells), F32)
    sums = (zero,) if mode == "right" else (zero, zero)
    sums = loop(REACH, rows - REACH, 4, update, sums)
    sums = [jnp.sum(jnp.sum(s, axis=1, keepdims=True), axis=0, keepdims=True) for s in sums]
    now = 1 - now

    back = back_ref[...]
    top, rest = halves(back)
    back = jnp.where(iota(back.shape, 0) < SUB, top, rest).astype(BF16)

    def look(field, w):
        def body(row, carry):
            top, rest = halves(field[row + HALO, :, :lon_cells])
            both = dot(back, jnp.concatenate([top, rest], axis=0).astype(BF16))
            typed = both[:SUB] + both[SUB:]
            for c in range(cols):
                at = pl.multiple_of(((w * lat_cells + row) * cols + c) * SUB, SUB)
                picked[pl.ds(at, SUB), :] = typed[:, c * LANES : (c + 1) * LANES]
            return carry

        loop(0, lat_cells, 8, body)

    look(fields[now], 0)
    for step in range(1, REACH + 1):
        old, new = fields[now], fields[1 - now]

        def body(e, carry, old=old, new=new):
            tangent(old, e, put_in(new, e))
            return carry

        loop(REACH + step, rows - REACH - step, 2, body)
        now = 1 - now
        if step % STEP_WIN == 0:
            look(fields[now], step // STEP_WIN)

    spare = jnp.where(iota((1, LANES), 1) < LANES // 2, sums[0], sums[-1])
    top, rest = halves(picked[...])
    values = jnp.concatenate([top, rest], axis=1).astype(BF16)
    chunk = 2 * LANES
    parts = lat_cells * cols
    for c in range(pack.recv // chunk):
        send = send_ref[:, c * chunk : (c + 1) * chunk]
        pick = jnp.where(iota((LANES, chunk), 0) == (send & (LANES - 1)), 1.0, 0.0)
        pick = jnp.concatenate([pick, pick], axis=0).astype(BF16)
        high = send >> log2(LANES)
        every = dot(values, pick)
        typed = []
        for w in range(WIN):
            found = jnp.zeros((SUB, chunk), F32)
            for h in range(parts):
                at = (w * parts + h) * SUB
                found = jnp.where(high == h, every[at : at + SUB], found)
            typed.append(found)
        for t in range(chunk // LANES):
            lanes = slice(t * LANES, (t + 1) * LANES)
            pack.write(out_ref, [x[:, lanes] for x in typed], spare, c * (chunk // LANES) + t)


def call(kernel, out_shapes, args, places, scratch, limit=24):
    specs = [pl.BlockSpec(memory_space=place) for place in places]
    specs += [pl.BlockSpec(memory_space=pltpu.VMEM)] * (len(args) - len(places))
    return pl.pallas_call(
        kernel,
        out_shape=[
            jax.ShapeDtypeStruct(s, F32) if isinstance(s, tuple) else s for s in out_shapes
        ],
        in_specs=specs,
        out_specs=[pl.BlockSpec(memory_space=pltpu.VMEM)] * len(out_shapes),
        scratch_shapes=[pltpu.VMEM(s, F32) if isinstance(s, tuple) else s for s in scratch],
        compiler_params=pltpu.CompilerParams(vmem_limit_bytes=limit << 20),
    )(*args)


def shards(
    zonal_wind,
    merid_wind,
    operator_rows,
    innovation,
    error_weight,
    interp_weight,
    obs_slot,
    block_count,
    block_type,
    block_window,
    send_cols,
):
    levels, lat_cells, lon_cells = zonal_wind.shape
    types, channels = operator_rows.shape
    layers = channels // levels
    n_lat, n_lon = lax.axis_size("lat"), lax.axis_size("lon")
    recv = send_cols.shape[1]
    blocks = block_count.shape[0]
    pack = Packing(n_lat * n_lon, recv)
    assert types == SUB and lat_cells >= HALO and lon_cells % LANES == 0
    assert recv % lon_cells == 0 and recv // lon_cells <= SUB
    dims = (layers, levels, lat_cells, lon_cells)
    width = lon_cells + LANES
    chunks = (pack.devices * pack.rows, LANES)
    block_args = [block_count, block_type, block_window]
    rows_of = lambda x: x.reshape(blocks, BLOCK_ROWS)
    error = rows_of(error_weight)
    total = (pack.rows, pack.devices, LANES)
    band = lax.axis_index("lat")
    edges = jnp.stack([band > 0, band < n_lat - 1]).astype(jnp.int32)
    into = jnp.tile(operator_rows.T, (1, 4))
    back = jnp.tile(operator_rows, (2, 2))

    def exchange(x):
        x = x.reshape(pack.devices * pack.rows, 1, LANES)
        x = lax.all_to_all(x, AXES, split_axis=0, concat_axis=0, tiled=True)
        return x.reshape(chunks)

    def send(x, up, right):
        pairs = [
            (i * n_lon + j, (i + up) % n_lat * n_lon + (j + right) % n_lon)
            for i in range(n_lat)
            for j in range(n_lon)
        ]
        return lax.ppermute(x, AXES, pairs)

    wind_slabs = 2 * lat_cells * (levels // SUB)

    def collect(received, halo, cells, with_winds=False):
        slabs = WIN * lat_cells + with_winds * wind_slabs
        strip = (SUB, -(-slabs * HALO // lon_cells) * lon_cells)
        main, west, east, energy = call(
            functools.partial(collect_kernel, pack, lat_cells, with_winds),
            [(slabs, SUB, lon_cells), strip, strip, (SUB, LANES)],
            [received, cells],
            [],
            [],
            16,
        )
        east, west = send(west, 0, -1), send(east, 0, 1)
        count = sum(trims(halo)) + slabs - WIN * lat_cells + 2 * strip[1] // lon_cells
        up, down = call(
            functools.partial(merge_kernel, halo, lat_cells),
            [(count, SUB, lon_cells)] * 2,
            [main, east, west],
            [],
            [],
        )
        return [send(up, 1, 0), main, send(down, -1, 0), east, west], energy

    def model(mode, halos, extra):
        ends = (channels * lat_cells, lon_cells)
        state = (lat_cells + 2 * REACH, channels, width)
        rows = lat_cells + 2 * (REACH if mode == "last" else HALO)
        outs = [ends, ends] if mode == "last" else [chunks, state]
        scratch = [(rows, channels, width)] * 2
        scratch += [(WIN, rows, SUB, width), (5, rows, levels, width)]
        if mode == "right":
            outs += [(2, rows, levels, width)]
        if mode == "last":
            scratch += [(ends[0], LANES)] * (2 * lon_cells // LANES)
        if mode != "last":
            scratch = [(WIN * lat_cells * lon_cells // LANES * SUB, LANES)] + scratch
        return call(
            functools.partial(model_kernel, pack, mode, dims),
            outs,
            [edges, *halos, into, back, *extra],
            [pltpu.SMEM],
            scratch,
        )

    def observe(mode, received, extra):
        outs, scratch = [chunks], [total]
        args = block_args + received + [obs_slot, interp_weight, error] + extra
        if mode == "right":
            places, limit = [pl.ANY] * len(args), 56
            strip = -(-(WIN * lat_cells + wind_slabs) * HALO // lon_cells)
            outs += [(wind_slabs + 2 * strip + 1, SUB, lon_cells)]
            scratch += [pltpu.SMEM(x.shape, x.dtype) for x in args[:3]]
            scratch += [pltpu.VMEM(x.shape, x.dtype) for x in args[3:]]
            scratch += [(levels * lat_cells, LANES)] * (lon_cells // LANES)
            scratch += [pltpu.SemaphoreType.DMA((len(args),))]
        else:
            places, limit = [pltpu.SMEM] * 3, 12
            outs += [(blocks, BLOCK_ROWS), (SUB, LANES)]
            scratch += [total]
        kernel = functools.partial(observe_kernel, pack, mode, lat_cells)
        return call(kernel, outs, args, places, scratch, limit)

    assert ITERS == 2
    winds = [x.reshape(levels * lat_cells, lon_cells) for x in (zonal_wind, merid_wind)]
    chunk, winds = observe("right", [], [rows_of(innovation), *winds, send_cols])
    halos, _ = collect(exchange(chunk), HALO, winds, True)
    chunk, right, winds = model("right", halos, [send_cols])
    chunk, seen, scalar0 = observe("start", [exchange(chunk)], [])
    halos, energy0 = collect(exchange(chunk), HALO, send_cols)
    chunk, residual = model("next", halos, [winds, energy0, scalar0, right, send_cols])
    chunk, seen, scalar1 = observe("next", [exchange(chunk)], [seen, scalar0])
    halos, energy1 = collect(exchange(chunk), REACH, send_cols)
    ends = model(
        "last", halos, [winds, energy1, scalar1, residual, energy0, scalar0, right]
    )
    return tuple(x.reshape(layers, levels, lat_cells, lon_cells) for x in ends)


def solution(mesh):
    return jax.shard_map(
        shards,
        mesh=mesh,
        in_specs=(
            P(None, "lat", "lon"),
            P(None, "lat", "lon"),
            P(),
            P(("lat", "lon")),
            P(("lat", "lon")),
            P(None, ("lat", "lon")),
            P(None, ("lat", "lon")),
            P(("lat", "lon")),
            P(("lat", "lon")),
            P(("lat", "lon")),
            P(("lat", "lon"), None),
        ),
        out_specs=(P(None, None, "lat", "lon"), P(None, None, "lat", "lon")),
        check_vma=False,
    )
```

```python
import functools

import jax
import jax.numpy as jnp
from jax import lax
from jax.experimental import pallas as pl
from jax.experimental.pallas import tpu as pltpu
from jax.sharding import PartitionSpec as P

WIN = 3
STEP_WIN = 2
ITERS = 2
BLOCK_ROWS = 128
LANES = 128
SUB = 8
REACH = STEP_WIN * (WIN - 1)
HALO = 2 * REACH
AXES = ("lat", "lon")
F32 = jnp.float32
BF16 = jnp.bfloat16
NT = (((1,), (1,)), ((), ()))


def log2(n):
    assert n & (n - 1) == 0
    return n.bit_length() - 1


def iota(shape, dim):
    return lax.broadcasted_iota(jnp.int32, shape, dim)


def halves(x):
    top = x.astype(BF16).astype(F32)
    return top, x - top


def dot(a, b):
    return jnp.dot(a, b, preferred_element_type=F32)


def loop(low, high, step, body, carry=0):
    count = high - low
    while count % step:
        step -= 1

    def some(i, carry):
        for k in range(step):
            carry = body(low + i * step + k, carry)
        return carry

    return lax.fori_loop(0, count // step, some, carry)


def trims(halo):
    return [max(halo - STEP_WIN * (WIN - 1 - w), 0) for w in range(WIN)]


class Packing:
    def __init__(self, devices, recv):
        self.devices = devices
        self.recv = recv
        self.slots = recv // devices
        assert self.slots <= LANES and recv % LANES == 0
        self.per = LANES // self.slots
        self.full = WIN // self.per
        self.left = WIN - self.full * self.per
        self.short = -(-self.left * SUB // self.per)
        self.spare = self.full * SUB + self.short
        self.rows = self.spare + 1
        self.group_bits = log2(self.slots)

    def group(self, shape):
        return iota(shape, len(shape) - 1) >> self.group_bits

    def place(self, window, kind):
        row = (window >> log2(self.per)) * SUB + kind
        group = window & (self.per - 1)
        if self.left:
            at = (window - self.full * self.per) * SUB + kind
            late = window >= self.full * self.per
            row = jnp.where(late, self.full * SUB + lax.rem(at, self.short), row)
            group = jnp.where(late, lax.div(at, self.short), group)
        return row, group * self.slots

    def sums(self, row):
        total = jnp.sum(row, axis=0, keepdims=True)
        lane = iota(total.shape, 1)
        return [
            jnp.sum(jnp.where(lane == at, total, 0.0), axis=1, keepdims=True)
            for at in (0, LANES // 2)
        ]

    def write(self, out_ref, typed, spare, tile):
        late = typed[self.full * self.per :]
        late = late[0] if len(late) == 1 else jnp.concatenate(late, axis=0)
        for d in range(self.per):
            base = (tile * self.per + d) * self.rows
            for part in range(self.full):
                chunk = None
                for g in range(self.per):
                    piece = turn(typed[part * self.per + g], (g - d) * self.slots)
                    chunk = piece if g == 0 else self.select(g, piece, chunk)
                out_ref[base + part * SUB : base + (part + 1) * SUB, :] = chunk
            chunk = jnp.zeros((self.short, LANES), F32)
            for g in range(self.per):
                piece = turn(late, (g - d) * self.slots)
                piece = piece[g * self.short : (g + 1) * self.short]
                chunk = piece if g == 0 else self.select(g, piece, chunk)
            base += self.full * SUB
            out_ref[base : base + self.short, :] = chunk
            out_ref[base + self.short : base + self.short + 1, :] = spare

    def select(self, group, yes, no):
        return jnp.where(self.group(yes.shape) == group, yes, no)

    def read(self, ref, tile):
        typed = [None] * WIN
        for d in range(self.per):
            base = (tile * self.per + d) * self.rows
            for part in range(self.full):
                piece = ref[base + part * SUB : base + (part + 1) * SUB, :]
                for g in range(self.per):
                    w = part * self.per + g
                    found = turn(piece, (d - g) * self.slots)
                    typed[w] = found if d == 0 else self.select(d, found, typed[w])
            base += self.full * SUB
            piece = ref[base : base + self.short, :]
            late = [turn(piece, (d - g) * self.slots) for g in range(self.per)]
            late = jnp.concatenate(late, axis=0)
            for i in range(self.left):
                w = self.full * self.per + i
                found = late[i * SUB : (i + 1) * SUB]
                typed[w] = found if d == 0 else self.select(d, found, typed[w])
        return typed


def turn(x, shift):
    shift %= x.shape[-1]
    return pltpu.roll(x, shift, len(x.shape) - 1) if shift else x


def note(strips, slab, left, right):
    q, s = slab * HALO // LANES, slab * HALO % LANES
    lane = iota((SUB, LANES), 1)
    inside = (lane >= s) & (lane < s + HALO)
    west, east = strips.get(q, (jnp.zeros((SUB, LANES), F32),) * 2)
    west = jnp.where(inside, turn(left, s), west)
    east = jnp.where(inside, turn(right, s - (LANES - HALO)), east)
    strips[q] = (west, east)


def lay_winds(first, refs, held, out_ref):
    cols, lat_cells = len(held), first // WIN
    slab, strips = 0, {}
    for ref in refs:
        for c in range(cols):
            held[c][...] = ref[:, c * LANES : (c + 1) * LANES]
        for row in range(lat_cells):
            for part in range(ref.shape[0] // lat_cells // SUB):
                at = pl.ds(part * SUB * lat_cells + row, SUB, stride=lat_cells)
                pieces = [held[c][at, :] for c in range(cols)]
                for c in range(cols):
                    out_ref[slab, :, c * LANES : (c + 1) * LANES] = pieces[c]
                note(strips, first + slab, pieces[0], pieces[-1])
                slab += 1
    count = (out_ref.shape[0] - 1 - slab) // 2
    for q in range(count * cols):
        for side in range(2):
            piece = strips[q][side] if q in strips else jnp.zeros((SUB, LANES), F32)
            lanes = slice(q % cols * LANES, (q % cols + 1) * LANES)
            out_ref[slab + side * count + q // cols, :, lanes] = piece


def observe_kernel(pack, mode, lat_cells, count_ref, type_ref, window_ref, *refs):
    if mode == "right":
        far = (count_ref, type_ref, window_ref) + refs[:7]
        out_ref, winds_ref, total = refs[7:10]
        near, held, done = refs[10:20], refs[20:-1], refs[-1]
        copies = [
            pltpu.make_async_copy(src, dst, done.at[i])
            for i, (src, dst) in enumerate(zip(far, near))
        ]
        for copy in copies:
            copy.start()
        total[...] = jnp.zeros_like(total)
        for copy in copies[:7]:
            copy.wait()
        count_ref, type_ref, window_ref, slot_ref, weight_ref, error_ref, value_ref = near[:7]
    else:
        if mode == "start":
            recv_ref, slot_ref, weight_ref, error_ref = refs[:4]
            refs = refs[4:]
        else:
            recv_ref, slot_ref, weight_ref, error_ref, value_ref, before_ref = refs[:6]
            refs = refs[6:]
        out_ref, observed_ref, scalar_ref, total, table = refs
    points = slot_ref.shape[0]
    blocks = error_ref.shape[0]
    devices = pack.devices
    wide = points * BLOCK_ROWS
    if mode != "right":
        total[...] = jnp.zeros_like(total)
        for j in range(pack.rows):
            table[j] = recv_ref[pl.ds(j, devices, stride=pack.rows), :]
        norm, cross = pack.sums(table[pack.spare])
        if mode == "start":
            ratio, square = jnp.zeros_like(norm), norm
        else:
            ratio = norm / before_ref[0:1, 0:1]
            square = norm + 2.0 * ratio * cross + ratio * ratio * before_ref[2:3, 0:1]
        row = iota((SUB, LANES), 0)
        scalar_ref[...] = jnp.where(row == 0, norm, jnp.where(row == 1, ratio, square))

    ids = iota((LANES, BLOCK_ROWS), 0)

    def row(x):
        return jnp.concatenate([x[k : k + 1, :] for k in range(points)], axis=1)

    def some(first, energy):
        group = [first * together + i for i in range(together)]
        places, picks, owners, weights, values = [], [], [], [], []
        for b in group:
            place, shift = pack.place(window_ref[b], type_ref[b])
            places.append(place)
            lanes = pl.ds(pl.multiple_of(b * BLOCK_ROWS, BLOCK_ROWS), BLOCK_ROWS)
            slot = slot_ref[:, lanes]
            lane = (slot & (pack.slots - 1)) + shift
            picks.append(
                jnp.concatenate(
                    [jnp.where(ids == lane[k : k + 1, :], 1.0, 0.0) for k in range(points)],
                    axis=1,
                ).astype(BF16)
            )
            owners.append(iota((devices, wide), 0) == row(slot >> pack.group_bits))
            weights.append(row(weight_ref[:, lanes]))
        if mode == "right":
            values = [value_ref[pl.ds(b, 1), :] for b in group]
        else:
            found = []
            for j, pick in zip(places, picks):
                top, rest = halves(table[j])
                found.append(dot(jnp.concatenate([top, rest], axis=0).astype(BF16), pick))
            for b, both, owner, weight in zip(group, found, owners, weights):
                both = both[:devices] + both[devices:]
                both = jnp.sum(jnp.where(owner, both, 0.0), axis=0, keepdims=True) * weight
                value = both[:, :BLOCK_ROWS]
                for k in range(1, points):
                    value = value + both[:, k * BLOCK_ROWS : (k + 1) * BLOCK_ROWS]
                if mode == "next":
                    value = value + ratio * value_ref[pl.ds(b, 1), :]
                values.append(value)
            for b, value in zip(group, values):
                observed_ref[pl.ds(b, 1), :] = value
        sums = []
        for b, pick, owner, weight, value in zip(group, picks, owners, weights, values):
            live = iota((1, BLOCK_ROWS), 1) < count_ref[b]
            weighted = jnp.where(live, error_ref[pl.ds(b, 1), :], 0.0) * value
            energy = energy + weighted * value
            spread = jnp.concatenate([weighted] * points, axis=1) * weight
            top, rest = halves(jnp.where(owner, spread, 0.0))
            sums.append(
                lax.dot_general(
                    jnp.concatenate([top, rest], axis=0).astype(BF16),
                    pick,
                    NT,
                    preferred_element_type=F32,
                )
            )
        for j, both in zip(places, sums):
            total[j] += both[:devices] + both[devices:]
        return energy

    together = 16 if mode == "right" else 8
    while blocks % together:
        together -= 1
    energy = jnp.zeros((1, BLOCK_ROWS), F32)
    energy = lax.fori_loop(0, blocks // together, some, energy)
    energy = jnp.sum(energy, axis=1, keepdims=True)
    for j in range(pack.rows):
        chunk = total[j]
        if j == pack.spare:
            chunk = jnp.broadcast_to(energy, (devices, LANES))
        out_ref[pl.ds(j, devices, stride=pack.rows), :] = chunk
    if mode == "right":
        for copy in copies[7:]:
            copy.wait()
        lay_winds(WIN * lat_cells, near[7:9], held, winds_ref)
        wide = winds_ref.shape[2]
        send = near[9][...].astype(F32)
        rows = [send[:, i * wide : (i + 1) * wide] for i in range(pack.recv // wide)]
        rows += [jnp.zeros((1, wide), F32)] * (SUB - len(rows))
        winds_ref[winds_ref.shape[0] - 1] = jnp.concatenate(rows, axis=0)


def collect_kernel(pack, lat_cells, with_winds, recv_ref, send_ref, *refs):
    main_ref, west_ref, east_ref, scalar_ref = refs
    lon_cells = main_ref.shape[2]
    cols = lon_cells // LANES
    tiles = pack.recv // LANES
    strips = {}
    if with_winds:
        send = send_ref[send_ref.shape[0] - 1]
        send = [send[i : i + 1] for i in range(pack.recv // lon_cells)]
        send = jnp.concatenate(send, axis=1).astype(jnp.int32)
        count = main_ref.shape[0] - WIN * lat_cells
        main_ref[WIN * lat_cells :] = send_ref[:count]
        half = west_ref.shape[1] // lon_cells
        for q in range(half * cols):
            lanes = slice(q % cols * LANES, (q % cols + 1) * LANES)
            at = count + q // cols
            strips[q] = (send_ref[at, :, lanes], send_ref[at + half, :, lanes])
    else:
        send = send_ref[...]
    pick = jnp.where(iota((LANES, pack.recv), 0) == (send & (LANES - 1)), 1.0, 0.0).astype(BF16)
    high = send >> log2(LANES)

    every = [pack.read(recv_ref, t) for t in range(tiles)]
    for w in range(WIN):
        typed = jnp.concatenate([x[w] for x in every], axis=1)
        masked = []
        for part in halves(typed):
            masked += [
                jnp.where(high == h, part, 0.0) for h in range(lat_cells * cols)
            ]
        both = lax.dot_general(
            jnp.concatenate(masked, axis=0).astype(BF16), pick, NT, preferred_element_type=F32
        )
        count = lat_cells * cols * SUB
        forcing = both[:count] + both[count:]
        for row in range(lat_cells):
            slab = w * lat_cells + row
            pieces = [
                forcing[(row * cols + c) * SUB : (row * cols + c + 1) * SUB] for c in range(cols)
            ]
            for c in range(cols):
                main_ref[slab, :, c * LANES : (c + 1) * LANES] = pieces[c]
            note(strips, slab, pieces[0], pieces[-1])
    for q in range(west_ref.shape[1] // LANES):
        west, east = strips[q]
        west_ref[:, q * LANES : (q + 1) * LANES] = west
        east_ref[:, q * LANES : (q + 1) * LANES] = east
    energy, _ = pack.sums(recv_ref[pl.ds(pack.spare, pack.devices, stride=pack.rows), :])
    scalar_ref[...] = jnp.broadcast_to(energy, scalar_ref.shape)


def merge_kernel(halo, lat_cells, main_ref, east_ref, west_ref, up_ref, down_ref):
    slab = 0
    for w, count in enumerate(trims(halo)):
        for row in range(count):
            up_ref[slab] = main_ref[w * lat_cells + lat_cells - count + row]
            down_ref[slab] = main_ref[w * lat_cells + row]
            slab += 1
    for at in range(WIN * lat_cells, main_ref.shape[0]):
        up_ref[slab] = main_ref[at]
        down_ref[slab] = main_ref[at]
        slab += 1
    wide = main_ref.shape[2]
    for ref in (east_ref, west_ref):
        for part in range(ref.shape[1] // wide):
            piece = ref[:, part * wide : (part + 1) * wide]
            up_ref[slab] = piece
            down_ref[slab] = piece
            slab += 1


def model_kernel(pack, mode, dims, edge_ref, *refs):
    layers, levels, lat_cells, lon_cells = dims
    channels = layers * levels
    halo = REACH if mode == "last" else HALO
    rows = lat_cells + 2 * halo
    cols = lon_cells // LANES
    width = lon_cells + LANES
    kept = trims(halo)
    refs = list(refs)

    def take(count):
        got = refs[:count]
        del refs[:count]
        return got

    south_ref, main_ref, north_ref, east_ref, west_ref = take(5)
    into_ref, back_ref = take(2)
    if mode != "right":
        (winds,) = take(1)
        energy_ref, scalar_ref, residual_ref = take(3)
    if mode == "last":
        (energy0_ref, scalar0_ref, first_ref) = take(3)
        increment_out, residual_out = take(2)
    else:
        (send_ref,) = take(1)
        out_ref, state_out = take(2)
        if mode == "right":
            (winds,) = take(1)
        (picked,) = take(1)
    fields = take(2)
    forced, coef = take(2)
    ends = refs

    lane = iota((SUB, LANES), 1)

    slabs = main_ref.shape[0]
    parts = east_ref.shape[1] // LANES
    beyond = [sum(kept) + slabs - WIN * lat_cells + i * (parts // cols) for i in range(2)]

    def assemble(slab, block, at):
        q, s = slab * HALO // LANES, slab * HALO % LANES
        if block == 1:
            main = main_ref[slab]
            east, west = (ref[:, q * LANES : (q + 1) * LANES] for ref in (east_ref, west_ref))
        else:
            ref = south_ref if block == 0 else north_ref
            main = ref[at]
            lanes = slice(q % cols * LANES, (q % cols + 1) * LANES)
            east, west = (ref[b + q // cols, :, lanes] for b in beyond)
        right = turn(east, -s)
        left = turn(west, LANES - HALO - s)
        edge = jnp.where(lane < HALO, right, jnp.where(lane >= LANES - HALO, left, 0.0))
        return jnp.concatenate([main, edge], axis=1)

    def source(e):
        at = e - halo
        if at < 0:
            return 0, lat_cells + at
        if at < lat_cells:
            return 1, at
        return 2, at - lat_cells

    for w in range(WIN):
        trim = halo - kept[w] if kept[w] else halo
        for e in range(trim, rows - trim):
            block, row = source(e)
            at = sum(kept[:w]) + (row - (lat_cells - kept[w]) if block == 0 else row)
            forced[w, e] = assemble(w * lat_cells + row, block, at)
    if mode == "right":
        for which in range(2):
            for e in range(rows):
                block, row = source(e)
                for part in range(levels // SUB):
                    at = (which * lat_cells + row) * (levels // SUB) + part
                    wind = assemble(WIN * lat_cells + at, block, sum(kept) + at)
                    if block != 1:
                        wind = jnp.where(edge_ref[block // 2] > 0, wind, 0.0)
                    winds[which, e, part * SUB : (part + 1) * SUB, :] = wind

    def prepare(e, carry):
        u, v = winds[0, e + HALO - halo], winds[1, e + HALO - halo]
        coef[0, e] = 1.0 - jnp.abs(u) - jnp.abs(v)
        coef[1, e] = jnp.maximum(u, 0.0)
        coef[2, e] = jnp.maximum(-u, 0.0)
        coef[3, e] = jnp.maximum(v, 0.0)
        coef[4, e] = jnp.maximum(-v, 0.0)
        return carry

    loop(0, rows, 8, prepare)

    into = into_ref[...]
    top, rest = halves(into)
    into = jnp.where(iota(into.shape, 1) < 2 * SUB, top, rest).astype(BF16)

    def force(w, e):
        top, rest = halves(forced[w, e])
        return dot(into, jnp.concatenate([top, rest, top, rest], axis=0).astype(BF16))

    def pieces(part):
        level = slice(part * SUB, (part + 1) * SUB)
        return level, [
            slice(v * levels + part * SUB, v * levels + (part + 1) * SUB) for v in range(layers)
        ]

    def adjoint(field, e, put, extra=None):
        for part in range(levels // SUB):
            level, chans = pieces(part)
            keep, west, east = coef[0, e, level], coef[1, e, level], coef[2, e, level]
            south, north = coef[3, e + 1, level], coef[4, e - 1, level]
            for chan in chans:
                here = field[e, chan]
                result = (
                    keep * here
                    + turn(west * here, -1)
                    + turn(east * here, 1)
                    + south * field[e + 1, chan]
                    + north * field[e - 1, chan]
                )
                if extra is not None:
                    result = result + extra[chan]
                put(chan, result)

    def tangent(field, e, put):
        for part in range(levels // SUB):
            level, chans = pieces(part)
            keep, west, east = coef[0, e, level], coef[1, e, level], coef[2, e, level]
            south, north = coef[3, e, level], coef[4, e, level]
            for chan in chans:
                here = field[e, chan]
                put(
                    chan,
                    keep * here
                    + west * turn(here, 1)
                    + east * turn(here, -1)
                    + south * field[e - 1, chan]
                    + north * field[e + 1, chan],
                )

    def put_in(field, e):
        def put(chan, value):
            field[e, chan] = value

        return put

    def begin(e, carry):
        fields[0][e] = force(WIN - 1, e)
        return carry

    loop(0, rows, 12, begin)
    now = 0
    for step in range(1, REACH):
        old, new = fields[now], fields[1 - now]
        w = WIN - 1 - step // STEP_WIN if step % STEP_WIN == 0 else None

        def body(e, carry, old=old, new=new, w=w):
            extra = None if w is None else force(w, e)
            adjoint(old, e, put_in(new, e), extra)
            return carry

        loop(step, rows - step, 11 if w is None else 10, body)
        now = 1 - now
    old, new = fields[now], fields[1 - now]

    if mode != "right":
        alpha = scalar_ref[0:1, 0:1] / (scalar_ref[2:3, 0:1] + energy_ref[0:1, 0:1])
        ratio = scalar_ref[1:2, 0:1]
    if mode == "last":
        alpha0 = scalar0_ref[0:1, 0:1] / (scalar0_ref[2:3, 0:1] + energy0_ref[0:1, 0:1])

        def finish(e, carry):
            row = e - halo

            def put(chan, value):
                at = pl.ds(chan.start * lat_cells + row, SUB, stride=lat_cells)
                for c in range(cols):
                    part = slice(c * LANES, (c + 1) * LANES)
                    residual = residual_ref[row + REACH, chan, part]
                    first = first_ref[row + REACH, chan, part]
                    direction = residual + ratio * first
                    image = direction + value[:, part]
                    ends[c][at, :] = alpha0 * first + alpha * direction
                    ends[cols + c][at, :] = residual - alpha * image

            adjoint(old, e, put, force(0, e))
            return carry

        loop(halo, halo + lat_cells, 8, finish)
        for c in range(cols):
            part = slice(c * LANES, (c + 1) * LANES)
            increment_out[:, part] = ends[c][...]
            residual_out[:, part] = ends[cols + c][...]
        return

    def update(e, sums):
        valid = jnp.where(e < HALO, edge_ref[0], jnp.where(e >= HALO + lat_cells, edge_ref[1], 1))
        scale = valid.astype(F32)
        inside = jnp.where((e >= HALO) & (e < HALO + lat_cells), 1, 0).astype(F32)
        at = e - REACH
        sums = list(sums)

        def put(chan, value):
            value = value * scale
            if mode != "right":
                before = residual_ref[at, chan]
                value = before - alpha * (before + value)
            state_out[at, chan] = value
            new[e, chan] = value
            kept = value[:, :lon_cells] * inside
            sums[0] = sums[0] + kept * value[:, :lon_cells]
            if mode != "right":
                sums[1] = sums[1] + kept * before[:, :lon_cells]

        adjoint(old, e, put, force(0, e))
        return tuple(sums)

    zero = jnp.zeros((SUB, lon_cells), F32)
    sums = (zero,) if mode == "right" else (zero, zero)
    sums = loop(REACH, rows - REACH, 8, update, sums)
    sums = [jnp.sum(jnp.sum(s, axis=1, keepdims=True), axis=0, keepdims=True) for s in sums]
    now = 1 - now

    back = back_ref[...]
    top, rest = halves(back)
    back = jnp.where(iota(back.shape, 0) < SUB, top, rest).astype(BF16)

    def look(field, w):
        def body(row, carry):
            top, rest = halves(field[row + HALO, :, :lon_cells])
            both = dot(back, jnp.concatenate([top, rest], axis=0).astype(BF16))
            typed = both[:SUB] + both[SUB:]
            for c in range(cols):
                at = pl.multiple_of(((w * lat_cells + row) * cols + c) * SUB, SUB)
                picked[pl.ds(at, SUB), :] = typed[:, c * LANES : (c + 1) * LANES]
            return carry

        loop(0, lat_cells, 8, body)

    look(fields[now], 0)
    for step in range(1, REACH + 1):
        old, new = fields[now], fields[1 - now]

        def body(e, carry, old=old, new=new):
            tangent(old, e, put_in(new, e))
            return carry

        loop(REACH + step, rows - REACH - step, 11, body)
        now = 1 - now
        if step % STEP_WIN == 0:
            look(fields[now], step // STEP_WIN)

    spare = jnp.where(iota((1, LANES), 1) < LANES // 2, sums[0], sums[-1])
    top, rest = halves(picked[...])
    values = jnp.concatenate([top, rest], axis=1).astype(BF16)
    chunk = 2 * LANES
    parts = lat_cells * cols
    for c in range(pack.recv // chunk):
        send = send_ref[:, c * chunk : (c + 1) * chunk]
        pick = jnp.where(iota((LANES, chunk), 0) == (send & (LANES - 1)), 1.0, 0.0)
        pick = jnp.concatenate([pick, pick], axis=0).astype(BF16)
        high = send >> log2(LANES)
        every = dot(values, pick)
        typed = []
        for w in range(WIN):
            found = jnp.zeros((SUB, chunk), F32)
            for h in range(parts):
                at = (w * parts + h) * SUB
                found = jnp.where(high == h, every[at : at + SUB], found)
            typed.append(found)
        for t in range(chunk // LANES):
            lanes = slice(t * LANES, (t + 1) * LANES)
            pack.write(out_ref, [x[:, lanes] for x in typed], spare, c * (chunk // LANES) + t)


def call(kernel, out_shapes, args, places, scratch, limit=24):
    specs = [pl.BlockSpec(memory_space=place) for place in places]
    specs += [pl.BlockSpec(memory_space=pltpu.VMEM)] * (len(args) - len(places))
    return pl.pallas_call(
        kernel,
        out_shape=[
            jax.ShapeDtypeStruct(s, F32) if isinstance(s, tuple) else s for s in out_shapes
        ],
        in_specs=specs,
        out_specs=[pl.BlockSpec(memory_space=pltpu.VMEM)] * len(out_shapes),
        scratch_shapes=[pltpu.VMEM(s, F32) if isinstance(s, tuple) else s for s in scratch],
        compiler_params=pltpu.CompilerParams(vmem_limit_bytes=limit << 20),
    )(*args)


def shards(
    zonal_wind,
    merid_wind,
    operator_rows,
    innovation,
    error_weight,
    interp_weight,
    obs_slot,
    block_count,
    block_type,
    block_window,
    send_cols,
):
    levels, lat_cells, lon_cells = zonal_wind.shape
    types, channels = operator_rows.shape
    layers = channels // levels
    n_lat, n_lon = lax.axis_size("lat"), lax.axis_size("lon")
    recv = send_cols.shape[1]
    blocks = block_count.shape[0]
    pack = Packing(n_lat * n_lon, recv)
    assert types == SUB and lat_cells >= HALO and lon_cells % LANES == 0
    assert recv % lon_cells == 0 and recv // lon_cells <= SUB
    dims = (layers, levels, lat_cells, lon_cells)
    width = lon_cells + LANES
    chunks = (pack.devices * pack.rows, LANES)
    block_args = [block_count, block_type, block_window]
    rows_of = lambda x: x.reshape(blocks, BLOCK_ROWS)
    error = rows_of(error_weight)
    total = (pack.rows, pack.devices, LANES)
    band = lax.axis_index("lat")
    edges = jnp.stack([band > 0, band < n_lat - 1]).astype(jnp.int32)
    into = jnp.tile(operator_rows.T, (1, 4))
    back = jnp.tile(operator_rows, (2, 2))

    def exchange(x):
        x = x.reshape(pack.devices * pack.rows, 1, LANES)
        x = lax.all_to_all(x, AXES, split_axis=0, concat_axis=0, tiled=True)
        return x.reshape(chunks)

    def send(x, up, right):
        pairs = [
            (i * n_lon + j, (i + up) % n_lat * n_lon + (j + right) % n_lon)
            for i in range(n_lat)
            for j in range(n_lon)
        ]
        return lax.ppermute(x, AXES, pairs)

    wind_slabs = 2 * lat_cells * (levels // SUB)

    def collect(received, halo, cells, with_winds=False):
        slabs = WIN * lat_cells + with_winds * wind_slabs
        strip = (SUB, -(-slabs * HALO // lon_cells) * lon_cells)
        main, west, east, energy = call(
            functools.partial(collect_kernel, pack, lat_cells, with_winds),
            [(slabs, SUB, lon_cells), strip, strip, (SUB, LANES)],
            [received, cells],
            [],
            [],
            16,
        )
        east, west = send(west, 0, -1), send(east, 0, 1)
        count = sum(trims(halo)) + slabs - WIN * lat_cells + 2 * strip[1] // lon_cells
        up, down = call(
            functools.partial(merge_kernel, halo, lat_cells),
            [(count, SUB, lon_cells)] * 2,
            [main, east, west],
            [],
            [],
        )
        return [send(up, 1, 0), main, send(down, -1, 0), east, west], energy

    def model(mode, halos, extra):
        ends = (channels * lat_cells, lon_cells)
        state = (lat_cells + 2 * REACH, channels, width)
        rows = lat_cells + 2 * (REACH if mode == "last" else HALO)
        outs = [ends, ends] if mode == "last" else [chunks, state]
        scratch = [(rows, channels, width)] * 2
        scratch += [(WIN, rows, SUB, width), (5, rows, levels, width)]
        if mode == "right":
            outs += [(2, rows, levels, width)]
        if mode == "last":
            scratch += [(ends[0], LANES)] * (2 * lon_cells // LANES)
        if mode != "last":
            scratch = [(WIN * lat_cells * lon_cells // LANES * SUB, LANES)] + scratch
        return call(
            functools.partial(model_kernel, pack, mode, dims),
            outs,
            [edges, *halos, into, back, *extra],
            [pltpu.SMEM],
            scratch,
        )

    def observe(mode, received, extra):
        outs, scratch = [chunks], [total]
        args = block_args + received + [obs_slot, interp_weight, error] + extra
        if mode == "right":
            places, limit = [pl.ANY] * len(args), 56
            strip = -(-(WIN * lat_cells + wind_slabs) * HALO // lon_cells)
            outs += [(wind_slabs + 2 * strip + 1, SUB, lon_cells)]
            scratch += [pltpu.SMEM(x.shape, x.dtype) for x in args[:3]]
            scratch += [pltpu.VMEM(x.shape, x.dtype) for x in args[3:]]
            scratch += [(levels * lat_cells, LANES)] * (lon_cells // LANES)
            scratch += [pltpu.SemaphoreType.DMA((len(args),))]
        else:
            places, limit = [pltpu.SMEM] * 3, 12
            outs += [(blocks, BLOCK_ROWS), (SUB, LANES)]
            scratch += [total]
        kernel = functools.partial(observe_kernel, pack, mode, lat_cells)
        return call(kernel, outs, args, places, scratch, limit)

    assert ITERS == 2
    winds = [x.reshape(levels * lat_cells, lon_cells) for x in (zonal_wind, merid_wind)]
    chunk, winds = observe("right", [], [rows_of(innovation), *winds, send_cols])
    halos, _ = collect(exchange(chunk), HALO, winds, True)
    chunk, right, winds = model("right", halos, [send_cols])
    chunk, seen, scalar0 = observe("start", [exchange(chunk)], [])
    halos, energy0 = collect(exchange(chunk), HALO, send_cols)
    chunk, residual = model("next", halos, [winds, energy0, scalar0, right, send_cols])
    chunk, seen, scalar1 = observe("next", [exchange(chunk)], [seen, scalar0])
    halos, energy1 = collect(exchange(chunk), REACH, send_cols)
    ends = model(
        "last", halos, [winds, energy1, scalar1, residual, energy0, scalar0, right]
    )
    return tuple(x.reshape(layers, levels, lat_cells, lon_cells) for x in ends)


def solution(mesh):
    return jax.shard_map(
        shards,
        mesh=mesh,
        in_specs=(
            P(None, "lat", "lon"),
            P(None, "lat", "lon"),
            P(),
            P(("lat", "lon")),
            P(("lat", "lon")),
            P(None, ("lat", "lon")),
            P(None, ("lat", "lon")),
            P(("lat", "lon")),
            P(("lat", "lon")),
            P(("lat", "lon")),
            P(("lat", "lon"), None),
        ),
        out_specs=(P(None, None, "lat", "lon"), P(None, None, "lat", "lon")),
        check_vma=False,
    )
```

```python
import functools

import jax
import jax.numpy as jnp
from jax import lax
from jax.experimental import pallas as pl
from jax.experimental.pallas import tpu as pltpu
from jax.sharding import PartitionSpec as P

WIN = 3
STEP_WIN = 2
ITERS = 2
BLOCK_ROWS = 128
LANES = 128
SUB = 8
REACH = STEP_WIN * (WIN - 1)
HALO = 2 * REACH
AXES = ("lat", "lon")
F32 = jnp.float32
BF16 = jnp.bfloat16
NT = (((1,), (1,)), ((), ()))


def log2(n):
    assert n & (n - 1) == 0
    return n.bit_length() - 1


def iota(shape, dim):
    return lax.broadcasted_iota(jnp.int32, shape, dim)


def halves(x):
    top = x.astype(BF16).astype(F32)
    return top, x - top


def dot(a, b):
    return jnp.dot(a, b, preferred_element_type=F32)


def loop(low, high, step, body, carry=0):
    count = high - low
    while count % step:
        step -= 1

    def some(i, carry):
        for k in range(step):
            carry = body(low + i * step + k, carry)
        return carry

    return lax.fori_loop(0, count // step, some, carry)


def trims(halo):
    return [max(halo - STEP_WIN * (WIN - 1 - w), 0) for w in range(WIN)]


class Packing:
    def __init__(self, devices, recv):
        self.devices = devices
        self.recv = recv
        self.slots = recv // devices
        assert self.slots <= LANES and recv % LANES == 0
        self.per = LANES // self.slots
        self.full = WIN // self.per
        self.left = WIN - self.full * self.per
        self.short = -(-self.left * SUB // self.per)
        self.spare = self.full * SUB + self.short
        self.rows = self.spare + 1
        self.group_bits = log2(self.slots)

    def group(self, shape):
        return iota(shape, len(shape) - 1) >> self.group_bits

    def place(self, window, kind):
        row = (window >> log2(self.per)) * SUB + kind
        group = window & (self.per - 1)
        if self.left:
            at = (window - self.full * self.per) * SUB + kind
            late = window >= self.full * self.per
            row = jnp.where(late, self.full * SUB + lax.rem(at, self.short), row)
            group = jnp.where(late, lax.div(at, self.short), group)
        return row, group * self.slots

    def sums(self, row):
        total = jnp.sum(row, axis=0, keepdims=True)
        lane = iota(total.shape, 1)
        return [
            jnp.sum(jnp.where(lane == at, total, 0.0), axis=1, keepdims=True)
            for at in (0, LANES // 2)
        ]

    def write(self, out_ref, typed, spare, tile):
        late = typed[self.full * self.per :]
        late = late[0] if len(late) == 1 else jnp.concatenate(late, axis=0)
        for d in range(self.per):
            base = (tile * self.per + d) * self.rows
            for part in range(self.full):
                chunk = None
                for g in range(self.per):
                    piece = turn(typed[part * self.per + g], (g - d) * self.slots)
                    chunk = piece if g == 0 else self.select(g, piece, chunk)
                out_ref[base + part * SUB : base + (part + 1) * SUB, :] = chunk
            chunk = jnp.zeros((self.short, LANES), F32)
            for g in range(self.per):
                piece = turn(late, (g - d) * self.slots)
                piece = piece[g * self.short : (g + 1) * self.short]
                chunk = piece if g == 0 else self.select(g, piece, chunk)
            base += self.full * SUB
            out_ref[base : base + self.short, :] = chunk
            out_ref[base + self.short : base + self.short + 1, :] = spare

    def select(self, group, yes, no):
        return jnp.where(self.group(yes.shape) == group, yes, no)

    def read(self, ref, tile):
        typed = [None] * WIN
        for d in range(self.per):
            base = (tile * self.per + d) * self.rows
            for part in range(self.full):
                piece = ref[base + part * SUB : base + (part + 1) * SUB, :]
                for g in range(self.per):
                    w = part * self.per + g
                    found = turn(piece, (d - g) * self.slots)
                    typed[w] = found if d == 0 else self.select(d, found, typed[w])
            base += self.full * SUB
            piece = ref[base : base + self.short, :]
            late = [turn(piece, (d - g) * self.slots) for g in range(self.per)]
            late = jnp.concatenate(late, axis=0)
            for i in range(self.left):
                w = self.full * self.per + i
                found = late[i * SUB : (i + 1) * SUB]
                typed[w] = found if d == 0 else self.select(d, found, typed[w])
        return typed


def one_hot(ids):
    rows = iota((LANES, ids.shape[1]), 0).astype(F32).astype(BF16)
    return jnp.where(rows == ids.astype(F32).astype(BF16), jnp.ones((), BF16), jnp.zeros((), BF16))


def turn(x, shift):
    shift %= x.shape[-1]
    return pltpu.roll(x, shift, len(x.shape) - 1) if shift else x


def note(strips, slab, left, right):
    q, s = slab * HALO // LANES, slab * HALO % LANES
    lane = iota((SUB, LANES), 1)
    inside = (lane >= s) & (lane < s + HALO)
    west, east = strips.get(q, (jnp.zeros((SUB, LANES), F32),) * 2)
    west = jnp.where(inside, turn(left, s), west)
    east = jnp.where(inside, turn(right, s - (LANES - HALO)), east)
    strips[q] = (west, east)


def lay_winds(first, refs, held, out_ref):
    cols, lat_cells = len(held), first // WIN
    slab, strips = 0, {}
    for ref in refs:
        for c in range(cols):
            held[c][...] = ref[:, c * LANES : (c + 1) * LANES]
        for row in range(lat_cells):
            for part in range(ref.shape[0] // lat_cells // SUB):
                at = pl.ds(part * SUB * lat_cells + row, SUB, stride=lat_cells)
                pieces = [held[c][at, :] for c in range(cols)]
                for c in range(cols):
                    out_ref[slab, :, c * LANES : (c + 1) * LANES] = pieces[c]
                note(strips, first + slab, pieces[0], pieces[-1])
                slab += 1
    count = (out_ref.shape[0] - 1 - slab) // 2
    for q in range(count * cols):
        for side in range(2):
            piece = strips[q][side] if q in strips else jnp.zeros((SUB, LANES), F32)
            lanes = slice(q % cols * LANES, (q % cols + 1) * LANES)
            out_ref[slab + side * count + q // cols, :, lanes] = piece


def observe_kernel(pack, mode, lat_cells, count_ref, type_ref, window_ref, *refs):
    if mode == "right":
        far = (count_ref, type_ref, window_ref) + refs[:7]
        out_ref, winds_ref, total = refs[7:10]
        near, held, done = refs[10:20], refs[20:-1], refs[-1]
        copies = [
            pltpu.make_async_copy(src, dst, done.at[i])
            for i, (src, dst) in enumerate(zip(far, near))
        ]
        for copy in copies:
            copy.start()
        total[...] = jnp.zeros_like(total)
        for copy in copies[:7]:
            copy.wait()
        count_ref, type_ref, window_ref, slot_ref, weight_ref, error_ref, value_ref = near[:7]
    else:
        if mode == "start":
            recv_ref, slot_ref, weight_ref, error_ref = refs[:4]
            refs = refs[4:]
        else:
            recv_ref, slot_ref, weight_ref, error_ref, value_ref, before_ref = refs[:6]
            refs = refs[6:]
        out_ref, observed_ref, scalar_ref, total, table = refs
    points = slot_ref.shape[0]
    blocks = error_ref.shape[0]
    devices = pack.devices
    wide = points * BLOCK_ROWS
    if mode != "right":
        total[...] = jnp.zeros_like(total)
        for j in range(pack.rows):
            table[j] = recv_ref[pl.ds(j, devices, stride=pack.rows), :]
        norm, cross = pack.sums(table[pack.spare])
        if mode == "start":
            ratio, square = jnp.zeros_like(norm), norm
        else:
            ratio = norm / before_ref[0:1, 0:1]
            square = norm + 2.0 * ratio * cross + ratio * ratio * before_ref[2:3, 0:1]
        row = iota((SUB, LANES), 0)
        scalar_ref[...] = jnp.where(row == 0, norm, jnp.where(row == 1, ratio, square))

    def row(x):
        return jnp.concatenate([x[k : k + 1, :] for k in range(points)], axis=1)

    def some(first, energy):
        group = [first * together + i for i in range(together)]
        places, picks, owners, weights, values = [], [], [], [], []
        for b in group:
            place, shift = pack.place(window_ref[b], type_ref[b])
            places.append(place)
            lanes = pl.ds(pl.multiple_of(b * BLOCK_ROWS, BLOCK_ROWS), BLOCK_ROWS)
            slot = slot_ref[:, lanes]
            lane = (slot & (pack.slots - 1)) + shift
            picks.append(one_hot(row(lane)))
            owners.append(iota((devices, wide), 0) == row(slot >> pack.group_bits))
            weights.append(row(weight_ref[:, lanes]))
        if mode == "right":
            values = [value_ref[pl.ds(b, 1), :] for b in group]
        else:
            found = []
            for j, pick in zip(places, picks):
                top, rest = halves(table[j])
                found.append(dot(jnp.concatenate([top, rest], axis=0).astype(BF16), pick))
            for b, both, owner, weight in zip(group, found, owners, weights):
                both = both[:devices] + both[devices:]
                both = jnp.sum(jnp.where(owner, both, 0.0), axis=0, keepdims=True) * weight
                value = both[:, :BLOCK_ROWS]
                for k in range(1, points):
                    value = value + both[:, k * BLOCK_ROWS : (k + 1) * BLOCK_ROWS]
                if mode == "next":
                    value = value + ratio * value_ref[pl.ds(b, 1), :]
                values.append(value)
            for b, value in zip(group, values):
                observed_ref[pl.ds(b, 1), :] = value
        sums = []
        for b, pick, owner, weight, value in zip(group, picks, owners, weights, values):
            live = iota((1, BLOCK_ROWS), 1) < count_ref[b]
            weighted = jnp.where(live, error_ref[pl.ds(b, 1), :], 0.0) * value
            energy = energy + weighted * value
            spread = jnp.concatenate([weighted] * points, axis=1) * weight
            top, rest = halves(jnp.where(owner, spread, 0.0))
            sums.append(
                lax.dot_general(
                    jnp.concatenate([top, rest], axis=0).astype(BF16),
                    pick,
                    NT,
                    preferred_element_type=F32,
                )
            )
        for j, both in zip(places, sums):
            total[j] += both[:devices] + both[devices:]
        return energy

    together = 16
    while blocks % together:
        together -= 1
    energy = jnp.zeros((1, BLOCK_ROWS), F32)
    energy = lax.fori_loop(0, blocks // together, some, energy)
    energy = jnp.sum(energy, axis=1, keepdims=True)
    for j in range(pack.rows):
        chunk = total[j]
        if j == pack.spare:
            chunk = jnp.broadcast_to(energy, (devices, LANES))
        out_ref[pl.ds(j, devices, stride=pack.rows), :] = chunk
    if mode == "right":
        for copy in copies[7:]:
            copy.wait()
        lay_winds(WIN * lat_cells, near[7:9], held, winds_ref)
        wide = winds_ref.shape[2]
        send = near[9][...].astype(F32)
        rows = [send[:, i * wide : (i + 1) * wide] for i in range(pack.recv // wide)]
        rows += [jnp.zeros((1, wide), F32)] * (SUB - len(rows))
        winds_ref[winds_ref.shape[0] - 1] = jnp.concatenate(rows, axis=0)


def collect_kernel(pack, lat_cells, with_winds, recv_ref, send_ref, *refs):
    main_ref, west_ref, east_ref, scalar_ref = refs
    lon_cells = main_ref.shape[2]
    cols = lon_cells // LANES
    tiles = pack.recv // LANES
    strips = {}
    if with_winds:
        send = send_ref[send_ref.shape[0] - 1]
        send = [send[i : i + 1] for i in range(pack.recv // lon_cells)]
        send = jnp.concatenate(send, axis=1).astype(jnp.int32)
        count = main_ref.shape[0] - WIN * lat_cells
        main_ref[WIN * lat_cells :] = send_ref[:count]
        half = west_ref.shape[1] // lon_cells
        for q in range(half * cols):
            lanes = slice(q % cols * LANES, (q % cols + 1) * LANES)
            at = count + q // cols
            strips[q] = (send_ref[at, :, lanes], send_ref[at + half, :, lanes])
    else:
        send = send_ref[...]
    pick = one_hot(send & (LANES - 1))
    high = send >> log2(LANES)

    every = [pack.read(recv_ref, t) for t in range(tiles)]
    for w in range(WIN):
        typed = jnp.concatenate([x[w] for x in every], axis=1)
        masked = []
        for part in halves(typed):
            masked += [
                jnp.where(high == h, part, 0.0) for h in range(lat_cells * cols)
            ]
        both = lax.dot_general(
            jnp.concatenate(masked, axis=0).astype(BF16), pick, NT, preferred_element_type=F32
        )
        count = lat_cells * cols * SUB
        forcing = both[:count] + both[count:]
        for row in range(lat_cells):
            slab = w * lat_cells + row
            pieces = [
                forcing[(row * cols + c) * SUB : (row * cols + c + 1) * SUB] for c in range(cols)
            ]
            for c in range(cols):
                main_ref[slab, :, c * LANES : (c + 1) * LANES] = pieces[c]
            note(strips, slab, pieces[0], pieces[-1])
    for q in range(west_ref.shape[1] // LANES):
        west, east = strips[q]
        west_ref[:, q * LANES : (q + 1) * LANES] = west
        east_ref[:, q * LANES : (q + 1) * LANES] = east
    energy, _ = pack.sums(recv_ref[pl.ds(pack.spare, pack.devices, stride=pack.rows), :])
    scalar_ref[...] = jnp.broadcast_to(energy, scalar_ref.shape)


def merge_kernel(halo, lat_cells, main_ref, east_ref, west_ref, up_ref, down_ref):
    slab = 0
    for w, count in enumerate(trims(halo)):
        for row in range(count):
            up_ref[slab] = main_ref[w * lat_cells + lat_cells - count + row]
            down_ref[slab] = main_ref[w * lat_cells + row]
            slab += 1
    for at in range(WIN * lat_cells, main_ref.shape[0]):
        up_ref[slab] = main_ref[at]
        down_ref[slab] = main_ref[at]
        slab += 1
    wide = main_ref.shape[2]
    for ref in (east_ref, west_ref):
        for part in range(ref.shape[1] // wide):
            piece = ref[:, part * wide : (part + 1) * wide]
            up_ref[slab] = piece
            down_ref[slab] = piece
            slab += 1


def model_kernel(pack, mode, dims, edge_ref, *refs):
    layers, levels, lat_cells, lon_cells = dims
    channels = layers * levels
    halo = REACH if mode == "last" else HALO
    rows = lat_cells + 2 * halo
    cols = lon_cells // LANES
    width = lon_cells + LANES
    kept = trims(halo)
    refs = list(refs)

    def take(count):
        got = refs[:count]
        del refs[:count]
        return got

    south_ref, main_ref, north_ref, east_ref, west_ref = take(5)
    into_ref, back_ref = take(2)
    if mode != "right":
        (winds,) = take(1)
        energy_ref, scalar_ref, residual_ref = take(3)
    if mode == "last":
        (energy0_ref, scalar0_ref, first_ref) = take(3)
        increment_out, residual_out = take(2)
    else:
        (send_ref,) = take(1)
        out_ref, state_out = take(2)
        if mode == "right":
            (winds,) = take(1)
        (picked,) = take(1)
    fields = take(2)
    forced, coef = take(2)
    ends = refs

    lane = iota((SUB, LANES), 1)

    slabs = main_ref.shape[0]
    parts = east_ref.shape[1] // LANES
    beyond = [sum(kept) + slabs - WIN * lat_cells + i * (parts // cols) for i in range(2)]

    def assemble(slab, block, at):
        q, s = slab * HALO // LANES, slab * HALO % LANES
        if block == 1:
            main = main_ref[slab]
            east, west = (ref[:, q * LANES : (q + 1) * LANES] for ref in (east_ref, west_ref))
        else:
            ref = south_ref if block == 0 else north_ref
            main = ref[at]
            lanes = slice(q % cols * LANES, (q % cols + 1) * LANES)
            east, west = (ref[b + q // cols, :, lanes] for b in beyond)
        right = turn(east, -s)
        left = turn(west, LANES - HALO - s)
        edge = jnp.where(lane < HALO, right, jnp.where(lane >= LANES - HALO, left, 0.0))
        return jnp.concatenate([main, edge], axis=1)

    def source(e):
        at = e - halo
        if at < 0:
            return 0, lat_cells + at
        if at < lat_cells:
            return 1, at
        return 2, at - lat_cells

    for w in range(WIN):
        trim = halo - kept[w] if kept[w] else halo
        for e in range(trim, rows - trim):
            block, row = source(e)
            at = sum(kept[:w]) + (row - (lat_cells - kept[w]) if block == 0 else row)
            forced[w, e] = assemble(w * lat_cells + row, block, at)
    if mode == "right":
        for which in range(2):
            for e in range(rows):
                block, row = source(e)
                for part in range(levels // SUB):
                    at = (which * lat_cells + row) * (levels // SUB) + part
                    wind = assemble(WIN * lat_cells + at, block, sum(kept) + at)
                    if block != 1:
                        wind = jnp.where(edge_ref[block // 2] > 0, wind, 0.0)
                    winds[which, e, part * SUB : (part + 1) * SUB, :] = wind

    def prepare(e, carry):
        u, v = winds[0, e + HALO - halo], winds[1, e + HALO - halo]
        coef[0, e] = 1.0 - jnp.abs(u) - jnp.abs(v)
        coef[1, e] = jnp.maximum(u, 0.0)
        coef[2, e] = jnp.maximum(-u, 0.0)
        coef[3, e] = jnp.maximum(v, 0.0)
        coef[4, e] = jnp.maximum(-v, 0.0)
        return carry

    loop(0, rows, 8, prepare)

    into = into_ref[...]
    top, rest = halves(into)
    into = jnp.where(iota(into.shape, 1) < 2 * SUB, top, rest).astype(BF16)

    def force(w, e):
        top, rest = halves(forced[w, e])
        return dot(into, jnp.concatenate([top, rest, top, rest], axis=0).astype(BF16))

    def pieces(part):
        level = slice(part * SUB, (part + 1) * SUB)
        return level, [
            slice(v * levels + part * SUB, v * levels + (part + 1) * SUB) for v in range(layers)
        ]

    def adjoint(field, e, put, extra=None):
        for part in range(levels // SUB):
            level, chans = pieces(part)
            keep, west, east = coef[0, e, level], coef[1, e, level], coef[2, e, level]
            south, north = coef[3, e + 1, level], coef[4, e - 1, level]
            for chan in chans:
                here = field[e, chan]
                result = (
                    keep * here
                    + turn(west * here, -1)
                    + turn(east * here, 1)
                    + south * field[e + 1, chan]
                    + north * field[e - 1, chan]
                )
                if extra is not None:
                    result = result + extra[chan]
                put(chan, result)

    def tangent(field, e, put):
        for part in range(levels // SUB):
            level, chans = pieces(part)
            keep, west, east = coef[0, e, level], coef[1, e, level], coef[2, e, level]
            south, north = coef[3, e, level], coef[4, e, level]
            for chan in chans:
                here = field[e, chan]
                put(
                    chan,
                    keep * here
                    + west * turn(here, 1)
                    + east * turn(here, -1)
                    + south * field[e - 1, chan]
                    + north * field[e + 1, chan],
                )

    def put_in(field, e):
        def put(chan, value):
            field[e, chan] = value

        return put

    def begin(e, carry):
        fields[0][e] = force(WIN - 1, e)
        return carry

    loop(0, rows, 12, begin)
    now = 0
    for step in range(1, REACH):
        old, new = fields[now], fields[1 - now]
        w = WIN - 1 - step // STEP_WIN if step % STEP_WIN == 0 else None

        def body(e, carry, old=old, new=new, w=w):
            extra = None if w is None else force(w, e)
            adjoint(old, e, put_in(new, e), extra)
            return carry

        loop(step, rows - step, 11 if w is None else 10, body)
        now = 1 - now
    old, new = fields[now], fields[1 - now]

    if mode != "right":
        alpha = scalar_ref[0:1, 0:1] / (scalar_ref[2:3, 0:1] + energy_ref[0:1, 0:1])
        ratio = scalar_ref[1:2, 0:1]
    if mode == "last":
        alpha0 = scalar0_ref[0:1, 0:1] / (scalar0_ref[2:3, 0:1] + energy0_ref[0:1, 0:1])

        def finish(e, carry):
            row = e - halo

            def put(chan, value):
                at = pl.ds(chan.start * lat_cells + row, SUB, stride=lat_cells)
                for c in range(cols):
                    part = slice(c * LANES, (c + 1) * LANES)
                    residual = residual_ref[row + REACH, chan, part]
                    first = first_ref[row + REACH, chan, part]
                    direction = residual + ratio * first
                    image = direction + value[:, part]
                    ends[c][at, :] = alpha0 * first + alpha * direction
                    ends[cols + c][at, :] = residual - alpha * image

            adjoint(old, e, put, force(0, e))
            return carry

        loop(halo, halo + lat_cells, 8, finish)
        for c in range(cols):
            part = slice(c * LANES, (c + 1) * LANES)
            increment_out[:, part] = ends[c][...]
            residual_out[:, part] = ends[cols + c][...]
        return

    def update(e, sums):
        valid = jnp.where(e < HALO, edge_ref[0], jnp.where(e >= HALO + lat_cells, edge_ref[1], 1))
        scale = valid.astype(F32)
        inside = jnp.where((e >= HALO) & (e < HALO + lat_cells), 1, 0).astype(F32)
        at = e - REACH
        sums = list(sums)

        def put(chan, value):
            value = value * scale
            if mode != "right":
                before = residual_ref[at, chan]
                value = before - alpha * (before + value)
            state_out[at, chan] = value
            new[e, chan] = value
            kept = value[:, :lon_cells] * inside
            sums[0] = sums[0] + kept * value[:, :lon_cells]
            if mode != "right":
                sums[1] = sums[1] + kept * before[:, :lon_cells]

        adjoint(old, e, put, force(0, e))
        return tuple(sums)

    zero = jnp.zeros((SUB, lon_cells), F32)
    sums = (zero,) if mode == "right" else (zero, zero)
    sums = loop(REACH, rows - REACH, 8, update, sums)
    sums = [jnp.sum(jnp.sum(s, axis=1, keepdims=True), axis=0, keepdims=True) for s in sums]
    now = 1 - now

    back = back_ref[...]
    top, rest = halves(back)
    back = jnp.where(iota(back.shape, 0) < SUB, top, rest).astype(BF16)

    def look(field, w):
        def body(row, carry):
            top, rest = halves(field[row + HALO, :, :lon_cells])
            both = dot(back, jnp.concatenate([top, rest], axis=0).astype(BF16))
            typed = both[:SUB] + both[SUB:]
            for c in range(cols):
                at = pl.multiple_of(((w * lat_cells + row) * cols + c) * SUB, SUB)
                picked[pl.ds(at, SUB), :] = typed[:, c * LANES : (c + 1) * LANES]
            return carry

        loop(0, lat_cells, 8, body)

    look(fields[now], 0)
    for step in range(1, REACH + 1):
        old, new = fields[now], fields[1 - now]

        def body(e, carry, old=old, new=new):
            tangent(old, e, put_in(new, e))
            return carry

        loop(REACH + step, rows - REACH - step, 11, body)
        now = 1 - now
        if step % STEP_WIN == 0:
            look(fields[now], step // STEP_WIN)

    spare = jnp.where(iota((1, LANES), 1) < LANES // 2, sums[0], sums[-1])
    top, rest = halves(picked[...])
    values = jnp.concatenate([top, rest], axis=1).astype(BF16)
    chunk = 4 * LANES
    parts = lat_cells * cols
    for c in range(pack.recv // chunk):
        send = send_ref[:, c * chunk : (c + 1) * chunk]
        pick = one_hot(send & (LANES - 1))
        pick = jnp.concatenate([pick, pick], axis=0)
        high = send >> log2(LANES)
        every = dot(values, pick)
        typed = []
        for w in range(WIN):
            found = jnp.zeros((SUB, chunk), F32)
            for h in range(parts):
                at = (w * parts + h) * SUB
                found = jnp.where(high == h, every[at : at + SUB], found)
            typed.append(found)
        for t in range(chunk // LANES):
            lanes = slice(t * LANES, (t + 1) * LANES)
            pack.write(out_ref, [x[:, lanes] for x in typed], spare, c * (chunk // LANES) + t)


def call(kernel, out_shapes, args, places, scratch, limit=24):
    specs = [pl.BlockSpec(memory_space=place) for place in places]
    specs += [pl.BlockSpec(memory_space=pltpu.VMEM)] * (len(args) - len(places))
    return pl.pallas_call(
        kernel,
        out_shape=[
            jax.ShapeDtypeStruct(s, F32) if isinstance(s, tuple) else s for s in out_shapes
        ],
        in_specs=specs,
        out_specs=[pl.BlockSpec(memory_space=pltpu.VMEM)] * len(out_shapes),
        scratch_shapes=[pltpu.VMEM(s, F32) if isinstance(s, tuple) else s for s in scratch],
        compiler_params=pltpu.CompilerParams(vmem_limit_bytes=limit << 20),
    )(*args)


def shards(
    zonal_wind,
    merid_wind,
    operator_rows,
    innovation,
    error_weight,
    interp_weight,
    obs_slot,
    block_count,
    block_type,
    block_window,
    send_cols,
):
    levels, lat_cells, lon_cells = zonal_wind.shape
    types, channels = operator_rows.shape
    layers = channels // levels
    n_lat, n_lon = lax.axis_size("lat"), lax.axis_size("lon")
    recv = send_cols.shape[1]
    blocks = block_count.shape[0]
    pack = Packing(n_lat * n_lon, recv)
    assert types == SUB and lat_cells >= HALO and lon_cells % LANES == 0
    assert recv % lon_cells == 0 and recv // lon_cells <= SUB
    dims = (layers, levels, lat_cells, lon_cells)
    width = lon_cells + LANES
    chunks = (pack.devices * pack.rows, LANES)
    block_args = [block_count, block_type, block_window]
    rows_of = lambda x: x.reshape(blocks, BLOCK_ROWS)
    error = rows_of(error_weight)
    total = (pack.rows, pack.devices, LANES)
    band = lax.axis_index("lat")
    edges = jnp.stack([band > 0, band < n_lat - 1]).astype(jnp.int32)
    into = jnp.tile(operator_rows.T, (1, 4))
    back = jnp.tile(operator_rows, (2, 2))

    def exchange(x):
        x = x.reshape(pack.devices * pack.rows, 1, LANES)
        x = lax.all_to_all(x, AXES, split_axis=0, concat_axis=0, tiled=True)
        return x.reshape(chunks)

    def send(x, up, right):
        pairs = [
            (i * n_lon + j, (i + up) % n_lat * n_lon + (j + right) % n_lon)
            for i in range(n_lat)
            for j in range(n_lon)
        ]
        return lax.ppermute(x, AXES, pairs)

    wind_slabs = 2 * lat_cells * (levels // SUB)

    def collect(received, halo, cells, with_winds=False):
        slabs = WIN * lat_cells + with_winds * wind_slabs
        strip = (SUB, -(-slabs * HALO // lon_cells) * lon_cells)
        main, west, east, energy = call(
            functools.partial(collect_kernel, pack, lat_cells, with_winds),
            [(slabs, SUB, lon_cells), strip, strip, (SUB, LANES)],
            [received, cells],
            [],
            [],
            16,
        )
        east, west = send(west, 0, -1), send(east, 0, 1)
        count = sum(trims(halo)) + slabs - WIN * lat_cells + 2 * strip[1] // lon_cells
        up, down = call(
            functools.partial(merge_kernel, halo, lat_cells),
            [(count, SUB, lon_cells)] * 2,
            [main, east, west],
            [],
            [],
        )
        return [send(up, 1, 0), main, send(down, -1, 0), east, west], energy

    def model(mode, halos, extra):
        ends = (channels * lat_cells, lon_cells)
        state = (lat_cells + 2 * REACH, channels, width)
        rows = lat_cells + 2 * (REACH if mode == "last" else HALO)
        outs = [ends, ends] if mode == "last" else [chunks, state]
        scratch = [(rows, channels, width)] * 2
        scratch += [(WIN, rows, SUB, width), (5, rows, levels, width)]
        if mode == "right":
            outs += [(2, rows, levels, width)]
        if mode == "last":
            scratch += [(ends[0], LANES)] * (2 * lon_cells // LANES)
        if mode != "last":
            scratch = [(WIN * lat_cells * lon_cells // LANES * SUB, LANES)] + scratch
        return call(
            functools.partial(model_kernel, pack, mode, dims),
            outs,
            [edges, *halos, into, back, *extra],
            [pltpu.SMEM],
            scratch,
        )

    def observe(mode, received, extra):
        outs, scratch = [chunks], [total]
        args = block_args + received + [obs_slot, interp_weight, error] + extra
        if mode == "right":
            places, limit = [pl.ANY] * len(args), 56
            strip = -(-(WIN * lat_cells + wind_slabs) * HALO // lon_cells)
            outs += [(wind_slabs + 2 * strip + 1, SUB, lon_cells)]
            scratch += [pltpu.SMEM(x.shape, x.dtype) for x in args[:3]]
            scratch += [pltpu.VMEM(x.shape, x.dtype) for x in args[3:]]
            scratch += [(levels * lat_cells, LANES)] * (lon_cells // LANES)
            scratch += [pltpu.SemaphoreType.DMA((len(args),))]
        else:
            places, limit = [pltpu.SMEM] * 3, 12
            outs += [(blocks, BLOCK_ROWS), (SUB, LANES)]
            scratch += [total]
        kernel = functools.partial(observe_kernel, pack, mode, lat_cells)
        return call(kernel, outs, args, places, scratch, limit)

    assert ITERS == 2
    winds = [x.reshape(levels * lat_cells, lon_cells) for x in (zonal_wind, merid_wind)]
    chunk, winds = observe("right", [], [rows_of(innovation), *winds, send_cols])
    halos, _ = collect(exchange(chunk), HALO, winds, True)
    chunk, right, winds = model("right", halos, [send_cols])
    chunk, seen, scalar0 = observe("start", [exchange(chunk)], [])
    halos, energy0 = collect(exchange(chunk), HALO, send_cols)
    chunk, residual = model("next", halos, [winds, energy0, scalar0, right, send_cols])
    chunk, seen, scalar1 = observe("next", [exchange(chunk)], [seen, scalar0])
    halos, energy1 = collect(exchange(chunk), REACH, send_cols)
    ends = model(
        "last", halos, [winds, energy1, scalar1, residual, energy0, scalar0, right]
    )
    return tuple(x.reshape(layers, levels, lat_cells, lon_cells) for x in ends)


def solution(mesh):
    return jax.shard_map(
        shards,
        mesh=mesh,
        in_specs=(
            P(None, "lat", "lon"),
            P(None, "lat", "lon"),
            P(),
            P(("lat", "lon")),
            P(("lat", "lon")),
            P(None, ("lat", "lon")),
            P(None, ("lat", "lon")),
            P(("lat", "lon")),
            P(("lat", "lon")),
            P(("lat", "lon")),
            P(("lat", "lon"), None),
        ),
        out_specs=(P(None, None, "lat", "lon"), P(None, None, "lat", "lon")),
        check_vma=False,
    )
```

```python
import functools

import jax
import jax.numpy as jnp
from jax import lax
from jax.experimental import pallas as pl
from jax.experimental.pallas import tpu as pltpu
from jax.sharding import PartitionSpec as P

WIN = 3
STEP_WIN = 2
ITERS = 2
BLOCK_ROWS = 128
LANES = 128
SUB = 8
REACH = STEP_WIN * (WIN - 1)
HALO = 2 * REACH
AXES = ("lat", "lon")
F32 = jnp.float32
BF16 = jnp.bfloat16
NT = (((1,), (1,)), ((), ()))


def log2(n):
    assert n & (n - 1) == 0
    return n.bit_length() - 1


def iota(shape, dim):
    return lax.broadcasted_iota(jnp.int32, shape, dim)


def halves(x):
    top = x.astype(BF16).astype(F32)
    return top, x - top


def dot(a, b):
    return jnp.dot(a, b, preferred_element_type=F32)


def loop(low, high, step, body, carry=0):
    count = high - low
    while count % step:
        step -= 1

    def some(i, carry):
        for k in range(step):
            carry = body(low + i * step + k, carry)
        return carry

    return lax.fori_loop(0, count // step, some, carry)


def trims(halo):
    return [max(halo - STEP_WIN * (WIN - 1 - w), 0) for w in range(WIN)]


class Packing:
    def __init__(self, devices, recv):
        self.devices = devices
        self.recv = recv
        self.slots = recv // devices
        assert self.slots <= LANES and recv % LANES == 0
        self.per = LANES // self.slots
        self.full = WIN // self.per
        self.left = WIN - self.full * self.per
        self.short = -(-self.left * SUB // self.per)
        self.spare = self.full * SUB + self.short
        self.rows = self.spare + 1
        self.group_bits = log2(self.slots)

    def group(self, shape):
        return iota(shape, len(shape) - 1) >> self.group_bits

    def place(self, window, kind):
        row = (window >> log2(self.per)) * SUB + kind
        group = window & (self.per - 1)
        if self.left:
            at = (window - self.full * self.per) * SUB + kind
            late = window >= self.full * self.per
            row = jnp.where(late, self.full * SUB + lax.rem(at, self.short), row)
            group = jnp.where(late, lax.div(at, self.short), group)
        return row, group * self.slots

    def sums(self, row):
        total = jnp.sum(row, axis=0, keepdims=True)
        lane = iota(total.shape, 1)
        return [
            jnp.sum(jnp.where(lane == at, total, 0.0), axis=1, keepdims=True)
            for at in (0, LANES // 2)
        ]

    def write(self, out_ref, typed, spare, tile):
        late = typed[self.full * self.per :]
        late = late[0] if len(late) == 1 else jnp.concatenate(late, axis=0)
        for d in range(self.per):
            base = (tile * self.per + d) * self.rows
            for part in range(self.full):
                chunk = None
                for g in range(self.per):
                    piece = turn(typed[part * self.per + g], (g - d) * self.slots)
                    chunk = piece if g == 0 else self.select(g, piece, chunk)
                out_ref[base + part * SUB : base + (part + 1) * SUB, :] = chunk
            chunk = jnp.zeros((self.short, LANES), F32)
            for g in range(self.per):
                piece = turn(late, (g - d) * self.slots)
                piece = piece[g * self.short : (g + 1) * self.short]
                chunk = piece if g == 0 else self.select(g, piece, chunk)
            base += self.full * SUB
            out_ref[base : base + self.short, :] = chunk
            out_ref[base + self.short : base + self.short + 1, :] = spare

    def select(self, group, yes, no):
        return jnp.where(self.group(yes.shape) == group, yes, no)

    def read(self, ref, tile):
        typed = [None] * WIN
        for d in range(self.per):
            base = (tile * self.per + d) * self.rows
            for part in range(self.full):
                piece = ref[base + part * SUB : base + (part + 1) * SUB, :]
                for g in range(self.per):
                    w = part * self.per + g
                    found = turn(piece, (d - g) * self.slots)
                    typed[w] = found if d == 0 else self.select(d, found, typed[w])
            base += self.full * SUB
            piece = ref[base : base + self.short, :]
            late = [turn(piece, (d - g) * self.slots) for g in range(self.per)]
            late = jnp.concatenate(late, axis=0)
            for i in range(self.left):
                w = self.full * self.per + i
                found = late[i * SUB : (i + 1) * SUB]
                typed[w] = found if d == 0 else self.select(d, found, typed[w])
        return typed


def one_hot(ids):
    rows = iota((LANES, ids.shape[1]), 0).astype(F32).astype(BF16)
    return jnp.where(rows == ids.astype(F32).astype(BF16), jnp.ones((), BF16), jnp.zeros((), BF16))


def turn(x, shift):
    shift %= x.shape[-1]
    return pltpu.roll(x, shift, len(x.shape) - 1) if shift else x


def note(strips, slab, left, right):
    q, s = slab * HALO // LANES, slab * HALO % LANES
    lane = iota((SUB, LANES), 1)
    inside = (lane >= s) & (lane < s + HALO)
    west, east = strips.get(q, (jnp.zeros((SUB, LANES), F32),) * 2)
    west = jnp.where(inside, turn(left, s), west)
    east = jnp.where(inside, turn(right, s - (LANES - HALO)), east)
    strips[q] = (west, east)


def lay_winds(first, refs, held, out_ref):
    cols, lat_cells = len(held), first // WIN
    slab, strips = 0, {}
    for ref in refs:
        for c in range(cols):
            held[c][...] = ref[:, c * LANES : (c + 1) * LANES]
        for row in range(lat_cells):
            for part in range(ref.shape[0] // lat_cells // SUB):
                at = pl.ds(part * SUB * lat_cells + row, SUB, stride=lat_cells)
                pieces = [held[c][at, :] for c in range(cols)]
                for c in range(cols):
                    out_ref[slab, :, c * LANES : (c + 1) * LANES] = pieces[c]
                note(strips, first + slab, pieces[0], pieces[-1])
                slab += 1
    count = (out_ref.shape[0] - 1 - slab) // 2
    for q in range(count * cols):
        for side in range(2):
            piece = strips[q][side] if q in strips else jnp.zeros((SUB, LANES), F32)
            lanes = slice(q % cols * LANES, (q % cols + 1) * LANES)
            out_ref[slab + side * count + q // cols, :, lanes] = piece


def observe_kernel(pack, mode, lat_cells, count_ref, type_ref, window_ref, *refs):
    if mode == "right":
        far = (count_ref, type_ref, window_ref) + refs[:7]
        out_ref, winds_ref, total = refs[7:10]
        near, held, done = refs[10:20], refs[20:-1], refs[-1]
        copies = [
            pltpu.make_async_copy(src, dst, done.at[i])
            for i, (src, dst) in enumerate(zip(far, near))
        ]
        for copy in copies:
            copy.start()
        total[...] = jnp.zeros_like(total)
        for copy in copies[:7]:
            copy.wait()
        count_ref, type_ref, window_ref, slot_ref, weight_ref, error_ref, value_ref = near[:7]
    else:
        if mode == "start":
            recv_ref, slot_ref, weight_ref, error_ref = refs[:4]
            refs = refs[4:]
        else:
            recv_ref, slot_ref, weight_ref, error_ref, value_ref, before_ref = refs[:6]
            refs = refs[6:]
        out_ref, observed_ref, scalar_ref, total, table = refs
    points = slot_ref.shape[0]
    blocks = error_ref.shape[0]
    devices = pack.devices
    wide = points * BLOCK_ROWS
    if mode != "right":
        total[...] = jnp.zeros_like(total)
        for j in range(pack.rows):
            table[j] = recv_ref[pl.ds(j, devices, stride=pack.rows), :]
        norm, cross = pack.sums(table[pack.spare])
        if mode == "start":
            ratio, square = jnp.zeros_like(norm), norm
        else:
            ratio = norm / before_ref[0:1, 0:1]
            square = norm + 2.0 * ratio * cross + ratio * ratio * before_ref[2:3, 0:1]
        row = iota((SUB, LANES), 0)
        scalar_ref[...] = jnp.where(row == 0, norm, jnp.where(row == 1, ratio, square))

    def row(x):
        return jnp.concatenate([x[k : k + 1, :] for k in range(points)], axis=1)

    def some(first, energy):
        group = [first * together + i for i in range(together)]
        places, picks, owners, weights, values = [], [], [], [], []
        for b in group:
            place, shift = pack.place(window_ref[b], type_ref[b])
            places.append(place)
            lanes = pl.ds(pl.multiple_of(b * BLOCK_ROWS, BLOCK_ROWS), BLOCK_ROWS)
            slot = slot_ref[:, lanes]
            lane = (slot & (pack.slots - 1)) + shift
            picks.append(one_hot(row(lane)))
            owners.append(iota((devices, wide), 0) == row(slot >> pack.group_bits))
            weights.append(row(weight_ref[:, lanes]))
        if mode == "right":
            values = [value_ref[pl.ds(b, 1), :] for b in group]
        else:
            found = []
            for j, pick in zip(places, picks):
                top, rest = halves(table[j])
                found.append(dot(jnp.concatenate([top, rest], axis=0).astype(BF16), pick))
            for b, both, owner, weight in zip(group, found, owners, weights):
                both = both[:devices] + both[devices:]
                both = jnp.sum(jnp.where(owner, both, 0.0), axis=0, keepdims=True) * weight
                value = both[:, :BLOCK_ROWS]
                for k in range(1, points):
                    value = value + both[:, k * BLOCK_ROWS : (k + 1) * BLOCK_ROWS]
                if mode == "next":
                    value = value + ratio * value_ref[pl.ds(b, 1), :]
                values.append(value)
            for b, value in zip(group, values):
                observed_ref[pl.ds(b, 1), :] = value
        sums = []
        for b, pick, owner, weight, value in zip(group, picks, owners, weights, values):
            live = iota((1, BLOCK_ROWS), 1) < count_ref[b]
            weighted = jnp.where(live, error_ref[pl.ds(b, 1), :], 0.0) * value
            energy = energy + weighted * value
            spread = jnp.concatenate([weighted] * points, axis=1) * weight
            top, rest = halves(jnp.where(owner, spread, 0.0))
            sums.append(
                lax.dot_general(
                    jnp.concatenate([top, rest], axis=0).astype(BF16),
                    pick,
                    NT,
                    preferred_element_type=F32,
                )
            )
        for j, both in zip(places, sums):
            total[j] += both[:devices] + both[devices:]
        return energy

    together = 16
    while blocks % together:
        together -= 1
    energy = jnp.zeros((1, BLOCK_ROWS), F32)
    energy = lax.fori_loop(0, blocks // together, some, energy)
    energy = jnp.sum(energy, axis=1, keepdims=True)
    for j in range(pack.rows):
        chunk = total[j]
        if j == pack.spare:
            chunk = jnp.broadcast_to(energy, (devices, LANES))
        out_ref[pl.ds(j, devices, stride=pack.rows), :] = chunk
    if mode == "right":
        for copy in copies[7:]:
            copy.wait()
        lay_winds(WIN * lat_cells, near[7:9], held, winds_ref)
        wide = winds_ref.shape[2]
        send = near[9][...].astype(F32)
        rows = [send[:, i * wide : (i + 1) * wide] for i in range(pack.recv // wide)]
        rows += [jnp.zeros((1, wide), F32)] * (SUB - len(rows))
        winds_ref[winds_ref.shape[0] - 1] = jnp.concatenate(rows, axis=0)


def collect_kernel(pack, lat_cells, with_winds, recv_ref, send_ref, *refs):
    main_ref, west_ref, east_ref, scalar_ref = refs
    lon_cells = main_ref.shape[2]
    cols = lon_cells // LANES
    tiles = pack.recv // LANES
    strips = {}
    if with_winds:
        send = send_ref[send_ref.shape[0] - 1]
        send = [send[i : i + 1] for i in range(pack.recv // lon_cells)]
        send = jnp.concatenate(send, axis=1).astype(jnp.int32)
        count = main_ref.shape[0] - WIN * lat_cells
        main_ref[WIN * lat_cells :] = send_ref[:count]
        half = west_ref.shape[1] // lon_cells
        for q in range(half * cols):
            lanes = slice(q % cols * LANES, (q % cols + 1) * LANES)
            at = count + q // cols
            strips[q] = (send_ref[at, :, lanes], send_ref[at + half, :, lanes])
    else:
        send = send_ref[...]
    pick = one_hot(send & (LANES - 1))
    high = send >> log2(LANES)

    every = [pack.read(recv_ref, t) for t in range(tiles)]
    for w in range(WIN):
        typed = jnp.concatenate([x[w] for x in every], axis=1)
        masked = []
        for part in halves(typed):
            masked += [
                jnp.where(high == h, part, 0.0) for h in range(lat_cells * cols)
            ]
        both = lax.dot_general(
            jnp.concatenate(masked, axis=0).astype(BF16), pick, NT, preferred_element_type=F32
        )
        count = lat_cells * cols * SUB
        forcing = both[:count] + both[count:]
        for row in range(lat_cells):
            slab = w * lat_cells + row
            pieces = [
                forcing[(row * cols + c) * SUB : (row * cols + c + 1) * SUB] for c in range(cols)
            ]
            for c in range(cols):
                main_ref[slab, :, c * LANES : (c + 1) * LANES] = pieces[c]
            note(strips, slab, pieces[0], pieces[-1])
    for q in range(west_ref.shape[1] // LANES):
        west, east = strips[q]
        west_ref[:, q * LANES : (q + 1) * LANES] = west
        east_ref[:, q * LANES : (q + 1) * LANES] = east
    energy, _ = pack.sums(recv_ref[pl.ds(pack.spare, pack.devices, stride=pack.rows), :])
    scalar_ref[...] = jnp.broadcast_to(energy, scalar_ref.shape)


def merge_kernel(halo, lat_cells, main_ref, east_ref, west_ref, up_ref, down_ref):
    slab = 0
    for w, count in enumerate(trims(halo)):
        for row in range(count):
            up_ref[slab] = main_ref[w * lat_cells + lat_cells - count + row]
            down_ref[slab] = main_ref[w * lat_cells + row]
            slab += 1
    for at in range(WIN * lat_cells, main_ref.shape[0]):
        up_ref[slab] = main_ref[at]
        down_ref[slab] = main_ref[at]
        slab += 1
    wide = main_ref.shape[2]
    for ref in (east_ref, west_ref):
        for part in range(ref.shape[1] // wide):
            piece = ref[:, part * wide : (part + 1) * wide]
            up_ref[slab] = piece
            down_ref[slab] = piece
            slab += 1


def model_kernel(pack, mode, dims, edge_ref, *refs):
    layers, levels, lat_cells, lon_cells = dims
    channels = layers * levels
    halo = REACH if mode == "last" else HALO
    rows = lat_cells + 2 * halo
    cols = lon_cells // LANES
    width = lon_cells + LANES
    kept = trims(halo)
    refs = list(refs)

    def take(count):
        got = refs[:count]
        del refs[:count]
        return got

    south_ref, main_ref, north_ref, east_ref, west_ref = take(5)
    into_ref, back_ref = take(2)
    if mode != "right":
        (winds,) = take(1)
        energy_ref, scalar_ref, residual_ref = take(3)
    if mode == "last":
        (energy0_ref, scalar0_ref, first_ref) = take(3)
        increment_out, residual_out = take(2)
    else:
        (send_ref,) = take(1)
        out_ref, state_out = take(2)
        if mode == "right":
            (winds,) = take(1)
        (picked,) = take(1)
    fields = take(2)
    forced, coef = take(2)
    ends = refs

    lane = iota((SUB, LANES), 1)

    slabs = main_ref.shape[0]
    parts = east_ref.shape[1] // LANES
    beyond = [sum(kept) + slabs - WIN * lat_cells + i * (parts // cols) for i in range(2)]

    def assemble(slab, block, at):
        q, s = slab * HALO // LANES, slab * HALO % LANES
        if block == 1:
            main = main_ref[slab]
            east, west = (ref[:, q * LANES : (q + 1) * LANES] for ref in (east_ref, west_ref))
        else:
            ref = south_ref if block == 0 else north_ref
            main = ref[at]
            lanes = slice(q % cols * LANES, (q % cols + 1) * LANES)
            east, west = (ref[b + q // cols, :, lanes] for b in beyond)
        right = turn(east, -s)
        left = turn(west, LANES - HALO - s)
        edge = jnp.where(lane < HALO, right, jnp.where(lane >= LANES - HALO, left, 0.0))
        return jnp.concatenate([main, edge], axis=1)

    def source(e):
        at = e - halo
        if at < 0:
            return 0, lat_cells + at
        if at < lat_cells:
            return 1, at
        return 2, at - lat_cells

    for w in range(WIN):
        trim = halo - kept[w] if kept[w] else halo
        for e in range(trim, rows - trim):
            block, row = source(e)
            at = sum(kept[:w]) + (row - (lat_cells - kept[w]) if block == 0 else row)
            forced[w, e] = assemble(w * lat_cells + row, block, at)
    if mode == "right":
        for which in range(2):
            for e in range(rows):
                block, row = source(e)
                for part in range(levels // SUB):
                    at = (which * lat_cells + row) * (levels // SUB) + part
                    wind = assemble(WIN * lat_cells + at, block, sum(kept) + at)
                    if block != 1:
                        wind = jnp.where(edge_ref[block // 2] > 0, wind, 0.0)
                    winds[which, e, part * SUB : (part + 1) * SUB, :] = wind

    def prepare(e, carry):
        u, v = winds[0, e + HALO - halo], winds[1, e + HALO - halo]
        coef[0, e] = 1.0 - jnp.abs(u) - jnp.abs(v)
        coef[1, e] = jnp.maximum(u, 0.0)
        coef[2, e] = jnp.maximum(-u, 0.0)
        coef[3, e] = jnp.maximum(v, 0.0)
        coef[4, e] = jnp.maximum(-v, 0.0)
        return carry

    loop(0, rows, 8, prepare)

    into = into_ref[...]
    top, rest = halves(into)
    into = jnp.where(iota(into.shape, 1) < 2 * SUB, top, rest).astype(BF16)

    def force(w, e):
        top, rest = halves(forced[w, e])
        return dot(into, jnp.concatenate([top, rest, top, rest], axis=0).astype(BF16))

    def pieces(part):
        level = slice(part * SUB, (part + 1) * SUB)
        return level, [
            slice(v * levels + part * SUB, v * levels + (part + 1) * SUB) for v in range(layers)
        ]

    def adjoint(field, e, put, extra=None):
        for part in range(levels // SUB):
            level, chans = pieces(part)
            keep, west, east = coef[0, e, level], coef[1, e, level], coef[2, e, level]
            south, north = coef[3, e + 1, level], coef[4, e - 1, level]
            for chan in chans:
                here = field[e, chan]
                result = (
                    keep * here
                    + turn(west * here, -1)
                    + turn(east * here, 1)
                    + south * field[e + 1, chan]
                    + north * field[e - 1, chan]
                )
                if extra is not None:
                    result = result + extra[chan]
                put(chan, result)

    def tangent(field, e, put):
        for part in range(levels // SUB):
            level, chans = pieces(part)
            keep, west, east = coef[0, e, level], coef[1, e, level], coef[2, e, level]
            south, north = coef[3, e, level], coef[4, e, level]
            for chan in chans:
                here = field[e, chan]
                put(
                    chan,
                    keep * here
                    + west * turn(here, 1)
                    + east * turn(here, -1)
                    + south * field[e - 1, chan]
                    + north * field[e + 1, chan],
                )

    def put_in(field, e):
        def put(chan, value):
            field[e, chan] = value

        return put

    def begin(e, carry):
        fields[0][e] = force(WIN - 1, e)
        return carry

    loop(0, rows, 12, begin)
    now = 0
    for step in range(1, REACH):
        old, new = fields[now], fields[1 - now]
        w = WIN - 1 - step // STEP_WIN if step % STEP_WIN == 0 else None

        def body(e, carry, old=old, new=new, w=w):
            extra = None if w is None else force(w, e)
            adjoint(old, e, put_in(new, e), extra)
            return carry

        loop(step, rows - step, 11 if w is None else 10, body)
        now = 1 - now
    old, new = fields[now], fields[1 - now]

    if mode != "right":
        alpha = scalar_ref[0:1, 0:1] / (scalar_ref[2:3, 0:1] + energy_ref[0:1, 0:1])
        ratio = scalar_ref[1:2, 0:1]
    if mode == "last":
        alpha0 = scalar0_ref[0:1, 0:1] / (scalar0_ref[2:3, 0:1] + energy0_ref[0:1, 0:1])

        def finish(e, carry):
            row = e - halo

            def put(chan, value):
                at = pl.ds(chan.start * lat_cells + row, SUB, stride=lat_cells)
                for c in range(cols):
                    part = slice(c * LANES, (c + 1) * LANES)
                    residual = residual_ref[row + REACH, chan, part]
                    first = first_ref[row + REACH, chan, part]
                    direction = residual + ratio * first
                    image = direction + value[:, part]
                    ends[c][at, :] = alpha0 * first + alpha * direction
                    ends[cols + c][at, :] = residual - alpha * image

            adjoint(old, e, put, force(0, e))
            return carry

        loop(halo, halo + lat_cells, 8, finish)
        for c in range(cols):
            part = slice(c * LANES, (c + 1) * LANES)
            increment_out[:, part] = ends[c][...]
            residual_out[:, part] = ends[cols + c][...]
        return

    def update(e, sums):
        valid = jnp.where(e < HALO, edge_ref[0], jnp.where(e >= HALO + lat_cells, edge_ref[1], 1))
        scale = valid.astype(F32)
        inside = jnp.where((e >= HALO) & (e < HALO + lat_cells), 1, 0).astype(F32)
        at = e - REACH
        sums = list(sums)

        def put(chan, value):
            value = value * scale
            if mode != "right":
                before = residual_ref[at, chan]
                value = before - alpha * (before + value)
            state_out[at, chan] = value
            new[e, chan] = value
            kept = value[:, :lon_cells] * inside
            sums[0] = sums[0] + kept * value[:, :lon_cells]
            if mode != "right":
                sums[1] = sums[1] + kept * before[:, :lon_cells]

        adjoint(old, e, put, force(0, e))
        return tuple(sums)

    zero = jnp.zeros((SUB, lon_cells), F32)
    sums = (zero,) if mode == "right" else (zero, zero)
    sums = loop(REACH, rows - REACH, 8, update, sums)
    sums = [jnp.sum(jnp.sum(s, axis=1, keepdims=True), axis=0, keepdims=True) for s in sums]
    now = 1 - now

    back = back_ref[...]
    top, rest = halves(back)
    back = jnp.where(iota(back.shape, 0) < SUB, top, rest).astype(BF16)

    def look(field, w):
        def body(row, carry):
            top, rest = halves(field[row + HALO, :, :lon_cells])
            both = dot(back, jnp.concatenate([top, rest], axis=0).astype(BF16))
            typed = both[:SUB] + both[SUB:]
            for c in range(cols):
                at = pl.multiple_of(((w * lat_cells + row) * cols + c) * SUB, SUB)
                picked[pl.ds(at, SUB), :] = typed[:, c * LANES : (c + 1) * LANES]
            return carry

        loop(0, lat_cells, 8, body)

    look(fields[now], 0)
    for step in range(1, REACH + 1):
        old, new = fields[now], fields[1 - now]

        def body(e, carry, old=old, new=new):
            tangent(old, e, put_in(new, e))
            return carry

        loop(REACH + step, rows - REACH - step, 14, body)
        now = 1 - now
        if step % STEP_WIN == 0:
            look(fields[now], step // STEP_WIN)

    spare = jnp.where(iota((1, LANES), 1) < LANES // 2, sums[0], sums[-1])
    top, rest = halves(picked[...])
    values = jnp.concatenate([top, rest], axis=1).astype(BF16)
    chunk = 4 * LANES
    parts = lat_cells * cols
    for c in range(pack.recv // chunk):
        send = send_ref[:, c * chunk : (c + 1) * chunk]
        pick = one_hot(send & (LANES - 1))
        pick = jnp.concatenate([pick, pick], axis=0)
        high = send >> log2(LANES)
        every = dot(values, pick)
        typed = []
        for w in range(WIN):
            found = jnp.zeros((SUB, chunk), F32)
            for h in range(parts):
                at = (w * parts + h) * SUB
                found = jnp.where(high == h, every[at : at + SUB], found)
            typed.append(found)
        for t in range(chunk // LANES):
            lanes = slice(t * LANES, (t + 1) * LANES)
            pack.write(out_ref, [x[:, lanes] for x in typed], spare, c * (chunk // LANES) + t)


def call(kernel, out_shapes, args, places, scratch, limit=24):
    specs = [pl.BlockSpec(memory_space=place) for place in places]
    specs += [pl.BlockSpec(memory_space=pltpu.VMEM)] * (len(args) - len(places))
    return pl.pallas_call(
        kernel,
        out_shape=[
            jax.ShapeDtypeStruct(s, F32) if isinstance(s, tuple) else s for s in out_shapes
        ],
        in_specs=specs,
        out_specs=[pl.BlockSpec(memory_space=pltpu.VMEM)] * len(out_shapes),
        scratch_shapes=[pltpu.VMEM(s, F32) if isinstance(s, tuple) else s for s in scratch],
        compiler_params=pltpu.CompilerParams(vmem_limit_bytes=limit << 20),
    )(*args)


def shards(
    zonal_wind,
    merid_wind,
    operator_rows,
    innovation,
    error_weight,
    interp_weight,
    obs_slot,
    block_count,
    block_type,
    block_window,
    send_cols,
):
    levels, lat_cells, lon_cells = zonal_wind.shape
    types, channels = operator_rows.shape
    layers = channels // levels
    n_lat, n_lon = lax.axis_size("lat"), lax.axis_size("lon")
    recv = send_cols.shape[1]
    blocks = block_count.shape[0]
    pack = Packing(n_lat * n_lon, recv)
    assert types == SUB and lat_cells >= HALO and lon_cells % LANES == 0
    assert recv % lon_cells == 0 and recv // lon_cells <= SUB
    dims = (layers, levels, lat_cells, lon_cells)
    width = lon_cells + LANES
    chunks = (pack.devices * pack.rows, LANES)
    block_args = [block_count, block_type, block_window]
    rows_of = lambda x: x.reshape(blocks, BLOCK_ROWS)
    error = rows_of(error_weight)
    total = (pack.rows, pack.devices, LANES)
    band = lax.axis_index("lat")
    edges = jnp.stack([band > 0, band < n_lat - 1]).astype(jnp.int32)
    into = jnp.tile(operator_rows.T, (1, 4))
    back = jnp.tile(operator_rows, (2, 2))

    def exchange(x):
        x = x.reshape(pack.devices * pack.rows, 1, LANES)
        x = lax.all_to_all(x, AXES, split_axis=0, concat_axis=0, tiled=True)
        return x.reshape(chunks)

    def send(x, up, right):
        pairs = [
            (i * n_lon + j, (i + up) % n_lat * n_lon + (j + right) % n_lon)
            for i in range(n_lat)
            for j in range(n_lon)
        ]
        return lax.ppermute(x, AXES, pairs)

    wind_slabs = 2 * lat_cells * (levels // SUB)

    def collect(received, halo, cells, with_winds=False):
        slabs = WIN * lat_cells + with_winds * wind_slabs
        strip = (SUB, -(-slabs * HALO // lon_cells) * lon_cells)
        main, west, east, energy = call(
            functools.partial(collect_kernel, pack, lat_cells, with_winds),
            [(slabs, SUB, lon_cells), strip, strip, (SUB, LANES)],
            [received, cells],
            [],
            [],
            16,
        )
        east, west = send(west, 0, -1), send(east, 0, 1)
        count = sum(trims(halo)) + slabs - WIN * lat_cells + 2 * strip[1] // lon_cells
        up, down = call(
            functools.partial(merge_kernel, halo, lat_cells),
            [(count, SUB, lon_cells)] * 2,
            [main, east, west],
            [],
            [],
        )
        return [send(up, 1, 0), main, send(down, -1, 0), east, west], energy

    def model(mode, halos, extra):
        ends = (channels * lat_cells, lon_cells)
        state = (lat_cells + 2 * REACH, channels, width)
        rows = lat_cells + 2 * (REACH if mode == "last" else HALO)
        outs = [ends, ends] if mode == "last" else [chunks, state]
        scratch = [(rows, channels, width)] * 2
        scratch += [(WIN, rows, SUB, width), (5, rows, levels, width)]
        if mode == "right":
            outs += [(2, rows, levels, width)]
        if mode == "last":
            scratch += [(ends[0], LANES)] * (2 * lon_cells // LANES)
        if mode != "last":
            scratch = [(WIN * lat_cells * lon_cells // LANES * SUB, LANES)] + scratch
        return call(
            functools.partial(model_kernel, pack, mode, dims),
            outs,
            [edges, *halos, into, back, *extra],
            [pltpu.SMEM],
            scratch,
        )

    def observe(mode, received, extra):
        outs, scratch = [chunks], [total]
        args = block_args + received + [obs_slot, interp_weight, error] + extra
        if mode == "right":
            places, limit = [pl.ANY] * len(args), 56
            strip = -(-(WIN * lat_cells + wind_slabs) * HALO // lon_cells)
            outs += [(wind_slabs + 2 * strip + 1, SUB, lon_cells)]
            scratch += [pltpu.SMEM(x.shape, x.dtype) for x in args[:3]]
            scratch += [pltpu.VMEM(x.shape, x.dtype) for x in args[3:]]
            scratch += [(levels * lat_cells, LANES)] * (lon_cells // LANES)
            scratch += [pltpu.SemaphoreType.DMA((len(args),))]
        else:
            places, limit = [pltpu.SMEM] * 3, 12
            outs += [(blocks, BLOCK_ROWS), (SUB, LANES)]
            scratch += [total]
        kernel = functools.partial(observe_kernel, pack, mode, lat_cells)
        return call(kernel, outs, args, places, scratch, limit)

    assert ITERS == 2
    winds = [x.reshape(levels * lat_cells, lon_cells) for x in (zonal_wind, merid_wind)]
    chunk, winds = observe("right", [], [rows_of(innovation), *winds, send_cols])
    halos, _ = collect(exchange(chunk), HALO, winds, True)
    chunk, right, winds = model("right", halos, [send_cols])
    chunk, seen, scalar0 = observe("start", [exchange(chunk)], [])
    halos, energy0 = collect(exchange(chunk), HALO, send_cols)
    chunk, residual = model("next", halos, [winds, energy0, scalar0, right, send_cols])
    chunk, seen, scalar1 = observe("next", [exchange(chunk)], [seen, scalar0])
    halos, energy1 = collect(exchange(chunk), REACH, send_cols)
    ends = model(
        "last", halos, [winds, energy1, scalar1, residual, energy0, scalar0, right]
    )
    return tuple(x.reshape(layers, levels, lat_cells, lon_cells) for x in ends)


def solution(mesh):
    return jax.shard_map(
        shards,
        mesh=mesh,
        in_specs=(
            P(None, "lat", "lon"),
            P(None, "lat", "lon"),
            P(),
            P(("lat", "lon")),
            P(("lat", "lon")),
            P(None, ("lat", "lon")),
            P(None, ("lat", "lon")),
            P(("lat", "lon")),
            P(("lat", "lon")),
            P(("lat", "lon")),
            P(("lat", "lon"), None),
        ),
        out_specs=(P(None, None, "lat", "lon"), P(None, None, "lat", "lon")),
        check_vma=False,
    )
```
